256 devices in a mesh: dp: 16 (over y, x_hi, core), proto: 16 (over x_lo, z).
Axes of the slice: x: 4 (x_hi: 2, x_lo: 2; x = x_hi * 2 + x_lo), y: 4, z: 8, core: 2. Of those that a mesh axis runs over, the one named last changes fastest.
Arguments:
- hidden_states: bfloat16 [512, 256, 2048], P(('dp', 'proto')), may hold values from -15 to 30, as said below
- teacher_feats: bfloat16 [512, 256, 384], P(('dp', 'proto')), may hold values from -25 to 25, as said below
- masks: int32 [512, 32], P(('dp', 'proto')), may hold values from 0 to 255, as said below
- head_weight: bfloat16 [2048, 384], replicated, as said below
- prototypes: bfloat16 [49152, 384], P('proto'), may hold values from -25 to 25, as said below
- center: float32 [49152], P('proto'), may hold values from -1.8 to 1.8
Outputs:
- loss: float32 [], replicated
- grad_hidden: bfloat16 [16384, 2048], P(('dp', 'proto'))
- grad_head: float32 [2048, 384], P(('dp', 'proto'))
The draws below stay inside these ranges and needn't reach their ends.
Inputs may be any that keep to these rules, and one draw needn't show every extreme that they name: `masks`: each row lists 32 different patch numbers of its image. `hidden_states`: independent entries. `teacher_feats`: independent entries. `head_weight`: independent entries of deviation 2048 ** -0.5. `prototypes`: independent entries.
All inputs are finite; a program needn't handle non-finite values.
Results may differ from the reference program's by a relative error of at most 0.00305.
The reference program's roundings to bfloat16 on the way (of `picked`, `student`, `teacher`, `grads` and `direction`) count: a program that leaves them out, or rounds other values in their place, can miss the bound.
Values may be sent and summed in bfloat16 or wider, within the bound.
A program may use at most 64 MiB of HBM per device.

```python
import math
import jax
import jax.numpy as jnp
from jax import lax

D_HID = 2048
D_BOT = 384
K = 49152
PATCHES = 256
MASK = 32
IMAGES = 512


def shared_law(key):
    base = jax.random.fold_in(key, 7771)
    weight = jnp.clip(jax.random.normal(jax.random.fold_in(base, 4), (D_HID, D_BOT), jnp.float32), -5.0, 5.0) / math.sqrt(D_HID)
    return weight


def draw_head_weight(key, part):
    return shared_law(key).astype(jnp.bfloat16)


def draw_prototypes(key, part):
    table = 0.2 * jnp.clip(jax.random.normal(jax.random.fold_in(key, 11), (K, D_BOT), jnp.float32), -5.0, 5.0)
    return table.astype(jnp.bfloat16)


def draw_hidden_states(key, part):
    states = jnp.clip(jax.random.normal(jax.random.fold_in(key, 21), (IMAGES, PATCHES, D_HID), jnp.float32), -5.0, 5.0)
    return states.astype(jnp.bfloat16)


def draw_teacher_feats(key, part):
    feats = jnp.clip(jax.random.normal(jax.random.fold_in(key, 31), (IMAGES, PATCHES, D_BOT), jnp.float32), -5.0, 5.0)
    return feats.astype(jnp.bfloat16)


def draw_masks(key, part):
    keys = jax.random.split(jax.random.fold_in(key, 3301), IMAGES)
    return jax.vmap(lambda single: jax.random.permutation(single, PATCHES)[:MASK])(keys).astype(jnp.int32)


def shard_levels(key, dims, pieces, least, high):
    loudness, own = 1.0, jax.random.fold_in(key, 6)
    for dim, parts in pieces:
        draws = jnp.exp(jax.random.uniform(jax.random.fold_in(own, dim), (parts,), jnp.float32, least / len(pieces), high / len(pieces)))
        loudness = loudness * jnp.repeat(draws, dims[dim] // parts).reshape([-1 if axis == dim else 1 for axis in range(len(dims))])
    return loudness


def bell_draw(stream_key, extent, spread, limit, cuts=(), kind=jnp.bfloat16):
    result = jax.random.normal(stream_key, extent, jnp.float32) * spread
    if len(cuts) > 0:
        result = shard_levels(stream_key, extent, cuts, -0.22, 0.18) * result
    return jnp.clip(result, min=-limit, max=limit).astype(kind)


def setup_inputs(seed: int = 0) -> dict:
    arg_keys = jax.random.split(jax.random.key(seed), 7)
    return {
        "hidden_states": draw_hidden_states(jax.random.fold_in(arg_keys[6], 71), 0),
        "teacher_feats": draw_teacher_feats(jax.random.fold_in(arg_keys[6], 71), 0),
        "masks": draw_masks(jax.random.fold_in(arg_keys[6], 71), 0),
        "head_weight": draw_head_weight(jax.random.fold_in(arg_keys[6], 71), 0),
        "prototypes": draw_prototypes(jax.random.fold_in(arg_keys[6], 71), 0),
        "center": bell_draw(arg_keys[5], (K,), 0.3, 1.8, ((0, 16),), jnp.float32),
    }


STUDENT_TEMP = 0.1
TEACHER_TEMP = 0.07
LOSS_SCALE = 524288.0
EPSILON = 1e-06

def unit_rows(feats):
    radius = jnp.sqrt(lax.optimization_barrier(jnp.sum(feats * feats, axis=-1, keepdims=True)) + EPSILON)
    return (feats / radius, radius)

def reference(hidden_states, teacher_feats, masks, head_weight, prototypes, center):
    picked = jnp.take_along_axis(hidden_states, masks[:, :, None], axis=1).reshape(-1, D_HID)
    teacher_rows = jnp.take_along_axis(teacher_feats, masks[:, :, None], axis=1).reshape(-1, D_BOT)
    raw = jnp.dot(picked.astype(jnp.float32), head_weight.astype(jnp.float32))
    unit, radius = unit_rows(raw)
    student = unit.astype(jnp.bfloat16)
    teacher = unit_rows(teacher_rows.astype(jnp.float32))[0].astype(jnp.bfloat16)
    table = prototypes.astype(jnp.float32)
    table_t = table.T
    total_rows = IMAGES * MASK
    factor = LOSS_SCALE / (total_rows * STUDENT_TEMP)
    width = math.gcd(total_rows, 256)

    def one_block(first):
        s_rows = lax.dynamic_slice_in_dim(student, first, width, 0).astype(jnp.float32)
        t_rows = lax.dynamic_slice_in_dim(teacher, first, width, 0).astype(jnp.float32)
        s_logits = jnp.dot(s_rows, table_t) / STUDENT_TEMP
        t_logits = (jnp.dot(t_rows, table_t) - center[None, :]) / TEACHER_TEMP
        peak_s = lax.optimization_barrier(jnp.max(s_logits, axis=1))
        s_weights = jnp.exp(s_logits - peak_s[:, None])
        total_s = lax.optimization_barrier(jnp.sum(s_weights, axis=1))
        peak_t = lax.optimization_barrier(jnp.max(t_logits, axis=1))
        t_weights = jnp.exp(t_logits - peak_t[:, None])
        total_t = lax.optimization_barrier(jnp.sum(t_weights, axis=1))
        cross = lax.optimization_barrier(jnp.sum(t_weights * s_logits, axis=1))
        row_loss = peak_s + jnp.log(total_s) - cross / total_t
        grads = (factor * (s_weights / total_s[:, None] - t_weights / total_t[:, None])).astype(jnp.bfloat16)
        back = jnp.dot(grads.astype(jnp.float32), table)
        return (row_loss, back)
    starts = jnp.arange(total_rows // width, dtype=jnp.int32) * width
    losses, backs = lax.map(one_block, starts)
    back = backs.reshape(total_rows, D_BOT)
    loss = jnp.sum(losses) / total_rows
    inner = lax.optimization_barrier(jnp.sum(unit * back, axis=-1, keepdims=True))
    direction = ((back - unit * inner) / radius).astype(jnp.bfloat16)
    grad_hidden = jnp.dot(direction.astype(jnp.float32), head_weight.astype(jnp.float32).T).astype(jnp.bfloat16)
    grad_head = jnp.dot(picked.astype(jnp.float32).T, direction.astype(jnp.float32))
    return (loss, grad_hidden, grad_head)
```

```python
import math

import jax
import jax.numpy as jnp
from jax import lax
from jax.experimental import pallas as pl
from jax.experimental.pallas import tpu as pltpu
from jax.sharding import Mesh
from jax.sharding import PartitionSpec as P

PROTO = ("proto_0", "proto_1")
DP_PROTO = ("dp", "proto_0", "proto_1")

STUDENT_TEMP = 0.1
TEACHER_TEMP = 0.07
LOSS_SCALE = 524288.0
EPSILON = 1e-06

LOG2E = 1.4426950408889634
LN2 = 0.6931471805599453
S_FACTOR = LOG2E / STUDENT_TEMP
T_FACTOR = LOG2E / TEACHER_TEMP

F32 = jnp.float32
BF16 = jnp.bfloat16
MESH = pl.DeviceIdType.MESH

DP = 16
NX = 2
NZ = 8
PEERS = NX * NZ
TILE = 512
KTILE = 1024


def contract(left, right, dims):
    return lax.dot_general(left, right, (dims, ((), ())), preferred_element_type=F32)


def kernel(
    masks,
    hidden_hbm,
    teacher_hbm,
    weight_hbm,
    protos_hbm,
    center,
    loss_out,
    hidden_out,
    head_out,
    hidden,
    feats,
    weight,
    protos,
    protos_t,
    centers,
    rows_all,
    s_all,
    t_all,
    unit_ref,
    radius_ref,
    picked_mine,
    picked_all,
    stats,
    stats_all,
    top,
    grads,
    total,
    parts,
    parts_all,
    dirs,
    losses,
    losses_p,
    heads,
    heads_all,
    load_sem,
    row_send,
    row_recv,
    pick_send,
    pick_recv,
    stat_send,
    stat_recv,
    part_send,
    part_recv,
    dir_send,
    dir_recv,
    pass_send,
    loss_send,
    loss_recv,
    lossp_send,
    lossp_recv,
    head_send,
    head_recv,
):
    d = lax.axis_index("dp")
    a = lax.axis_index("proto_0")
    z = lax.axis_index("proto_1")
    b = 1 - a
    p = a * NZ + z
    images, patches, _ = hidden.shape
    picks = masks.shape[1]
    rows = images * picks
    bottleneck = weight.shape[1]
    table = protos.shape[0]
    tiles = table // TILE
    lines = TILE // 8
    pending = []

    def send(src, dst, send_sem, recv_sem, device):
        copy = pltpu.make_async_remote_copy(
            src_ref=src,
            dst_ref=dst,
            send_sem=send_sem,
            recv_sem=recv_sem,
            device_id=device,
            device_id_type=MESH,
        )
        copy.start()
        pending.append(copy)

    def arrived(ref, sem):
        pltpu.make_async_remote_copy(
            src_ref=ref,
            dst_ref=ref,
            send_sem=sem,
            recv_sem=sem,
            device_id={"proto_0": b},
            device_id_type=MESH,
        ).wait_recv()

    def proto_peer(k):
        peer = (p + k) % PEERS
        return peer, {"proto_0": peer // NZ, "proto_1": peer % NZ}

    def dp_peer(k):
        peer = (d + k) % DP
        return peer, {"dp": peer}

    loads = [
        pltpu.make_async_copy(src, dst, load_sem.at[k])
        for k, (src, dst) in enumerate(
            (
                (hidden_hbm, hidden),
                (weight_hbm, weight),
                (teacher_hbm, feats),
                (protos_hbm, protos),
            )
        )
    ]
    for load in loads:
        load.start()

    barrier = pltpu.get_barrier_semaphore()
    for k in range(1, PEERS):
        pl.semaphore_signal(barrier, inc=1, device_id=proto_peer(k)[1], device_id_type=MESH)
    for k in range(1, DP):
        pl.semaphore_signal(barrier, inc=1, device_id=dp_peer(k)[1], device_id_type=MESH)

    loads[0].wait()
    loads[1].wait()
    loads[2].wait()
    picked_parts = []
    teacher_parts = []
    for image in range(images):
        index = lax.broadcasted_iota(jnp.int32, (patches, picks), 0)
        hot = (index == masks[image : image + 1, :]).astype(F32).astype(BF16)
        picked_parts.append(contract(hot, hidden[image], ((0,), (0,))).astype(BF16))
        teacher_parts.append(contract(hot, feats[image], ((0,), (0,))))
    picked = jnp.concatenate(picked_parts, axis=0)
    chosen = jnp.concatenate(teacher_parts, axis=0)
    raw = contract(picked, weight[...], ((1,), (0,)))
    radius = jnp.sqrt(jnp.sum(raw * raw, axis=1, keepdims=True) + EPSILON)
    unit = raw / radius
    unit_ref[...] = unit
    radius_ref[...] = jnp.broadcast_to(radius, radius_ref.shape)
    length = jnp.sqrt(jnp.sum(chosen * chosen, axis=1, keepdims=True) + EPSILON)
    rows_all[z, a] = unit.astype(BF16)
    rows_all[z, 2 + a] = (chosen / length).astype(BF16)
    share = picked_mine.shape[2]
    for k in range(DP):
        picked_mine[k] = picked[:, k * share : (k + 1) * share]

    pl.semaphore_wait(barrier, PEERS + DP - 2)

    above = {"proto_1": (z + 1) % NZ}
    below = {"proto_1": (z + NZ - 1) % NZ}
    beside = {"proto_0": b}
    row_count = []

    def at(step):
        return (z + step) % NZ

    def slot(other, step, kind):
        return at(step % NZ), (b if other else a) + 2 * kind

    def row_pass(other, step, kind, device):
        line, column = slot(other, step, kind)
        ref = rows_all.at[line, column]
        send(ref, ref, row_send.at[len(row_count)], row_recv.at[line, column], device)
        row_count.append(0)

    def row_wait(other, step, kind):
        line, column = slot(other, step, kind)
        arrived(rows_all.at[line, column], row_recv.at[line, column])

    for kind in (0, 1):
        row_pass(0, 0, kind, above)
        row_pass(0, 0, kind, below)
        row_pass(0, 0, kind, beside)

    for k in range(1, DP):
        peer, device = dp_peer(k)
        send(picked_mine.at[peer], picked_all.at[d], pick_send.at[k], pick_recv.at[d], device)
    picked_all[d] = picked_mine[d]

    loads[3].wait()

    def turn(index, _):
        first = pl.multiple_of(index * 256, 256)
        protos_t[index] = protos[pl.ds(first, 256), :].T
        return 0

    lax.fori_loop(0, table // 256, turn, 0)

    def spread(index, _):
        line = center[pl.ds(index, 1), :]
        column = jnp.broadcast_to(line, (128, 128)).T
        centers[pl.ds(index * 16, 16)] = column.reshape(16, 8, 128)
        return 0

    lax.fori_loop(0, table // 128, spread, 0)

    def down(ref):
        return jnp.broadcast_to(ref, (8, 128))

    def logits_tile(index, line, state):
        peak_s, peak_t = state
        first = pl.multiple_of(index * TILE, TILE)
        tile = protos[pl.ds(first, TILE), :]
        both = contract(tile, rows_all[line].reshape(4 * rows, bottleneck), ((1,), (1,)))
        at_line = pl.ds(index * lines, lines)
        s = both[:, : 2 * rows].reshape(lines, 8, 128)
        t = both[:, 2 * rows :].reshape(lines, 8, 128) - centers[at_line]
        s_all[line, at_line] = s
        t_all[line, at_line] = t
        return jnp.maximum(peak_s, jnp.max(s, axis=0)), jnp.maximum(peak_t, jnp.max(t, axis=0))

    def weights_tile(index, line, peaks, state):
        total_s, total_t, cross = state
        at_line = pl.ds(index * lines, lines)
        s = s_all[line, at_line]
        power_s = jnp.exp2((s - peaks[0]) * S_FACTOR)
        power_t = jnp.exp2((t_all[line, at_line] - peaks[1]) * T_FACTOR)
        s_all[line, at_line] = power_s
        t_all[line, at_line] = power_t
        return (
            total_s + jnp.sum(power_s, axis=0),
            total_t + jnp.sum(power_t, axis=0),
            cross + jnp.sum(power_t * s, axis=0),
        )

    lowest = (jnp.full((8, 128), -jnp.inf, F32),) * 2
    zeros = (jnp.zeros((8, 128), F32),) * 3

    def peaks_of(state):
        return tuple(down(jnp.max(part, axis=0, keepdims=True)) for part in state)

    def finish(line, peaks, state):
        total_s, total_t, cross = (jnp.sum(part, axis=0, keepdims=True) for part in state)
        here = pl.ds(line, 1)
        shift_s = peaks[0][:1] * S_FACTOR
        shift_t = peaks[1][:1] * T_FACTOR
        top[0, here, :] = shift_s
        top[1, here, :] = shift_t
        top[2, here, :] = cross / total_t
        stats[0, here, :] = shift_s + jnp.log(total_s) * LOG2E
        stats[1, here, :] = shift_t + jnp.log(total_t) * LOG2E

    def first_pair(line):
        return peaks_of(
            lax.fori_loop(0, tiles, lambda i, state: logits_tile(i, line, state), lowest)
        )

    def pair(line, before, peaks):
        def body(index, state):
            return (
                logits_tile(index, line, state[0]),
                weights_tile(index, before, peaks, state[1]),
            )

        new, sums = lax.fori_loop(0, tiles, body, (lowest, zeros))
        finish(before, peaks, sums)
        return peaks_of(new)

    def last_pair(before, peaks):
        sums = lax.fori_loop(
            0, tiles, lambda i, state: weights_tile(i, before, peaks, state), zeros
        )
        finish(before, peaks, sums)

    for kind in (0, 1):
        row_wait(0, 1, kind)
        row_pass(0, 1, kind, below)
        row_pass(0, 1, kind, beside)
        row_wait(0, -1, kind)
        row_pass(0, -1, kind, above)
        row_pass(0, -1, kind, beside)
    row_wait(1, 0, 0)
    row_wait(1, 0, 1)
    peaks = first_pair(at(0))
    for kind in (0, 1):
        row_wait(0, 2, kind)
        row_pass(0, 2, kind, below)
        row_pass(0, 2, kind, beside)
        row_wait(0, -2, kind)
        row_pass(0, -2, kind, above)
        row_pass(0, -2, kind, beside)
    row_wait(1, 1, 0)
    row_wait(1, 1, 1)
    peaks = pair(at(1), at(0), peaks)
    row_wait(1, -1, 0)
    row_wait(1, -1, 1)
    peaks = pair(at(7), at(1), peaks)
    for kind in (0, 1):
        row_wait(1, 2, kind)
        row_pass(1, 2, kind, below)
        row_wait(1, -2, kind)
        row_pass(1, -2, kind, above)
    row_wait(0, 3, 0)
    row_pass(0, 3, 0, below)
    row_wait(0, -3, 1)
    row_pass(0, -3, 1, above)
    peaks = pair(at(2), at(7), peaks)
    row_wait(1, 3, 0)
    row_pass(1, 3, 0, below)
    row_wait(1, -3, 1)
    row_pass(1, -3, 1, above)
    peaks = pair(at(6), at(2), peaks)
    row_wait(0, 3, 1)
    row_wait(1, 3, 1)
    peaks = pair(at(3), at(6), peaks)
    row_wait(0, -3, 0)
    row_wait(1, -3, 0)
    peaks = pair(at(5), at(3), peaks)
    for kind in (0, 1):
        row_wait(0, 4, kind)
        row_wait(1, 4, kind)
    peaks = pair(at(4), at(5), peaks)
    last_pair(at(4), peaks)

    for k in range(1, PEERS):
        peer, device = proto_peer(k)
        send(stats, stats_all.at[p], stat_send.at[k], stat_recv.at[p], device)
    stats_all[p] = stats[...]
    for k in range(1, PEERS):
        peer = (p + k) % PEERS
        arrived(stats_all.at[peer], stat_recv.at[peer])
    every = stats_all[...]
    highest = jnp.max(every, axis=0)
    joined = highest + jnp.log(jnp.sum(jnp.exp2(every - highest), axis=0)) * LOG2E
    total_rows = rows * PEERS * DP
    factor = math.log2(LOSS_SCALE / (total_rows * STUDENT_TEMP))
    losses[d] = joined[0] * (LN2 / PEERS) - top[2] * jnp.exp2(stats[1] - joined[1]) / STUDENT_TEMP
    top[0] = jnp.exp2(top[0] - joined[0] + factor)
    top[1] = jnp.exp2(top[1] - joined[1] + factor)

    def part_of(line, chunk):
        here = pl.ds(chunk * (KTILE // 8), KTILE // 8)
        up = down(top[0, pl.ds(line, 1), :])
        off = down(top[1, pl.ds(line, 1), :])
        value = s_all[line, here] * up - t_all[line, here] * off
        return value.reshape(KTILE, 128).astype(BF16)

    def back_of(far, near):
        for chunk in range(table // KTILE):
            grads[chunk, :, :128] = part_of(far, chunk)
            grads[chunk, :, 128:] = part_of(near, chunk)
        for chunk in range(table // KTILE):
            left = jnp.concatenate(
                [protos_t[chunk * (KTILE // 256) + k] for k in range(KTILE // 256)], axis=1
            )
            product = contract(left, grads[chunk], ((1,), (0,)))
            if chunk == 0:
                total[...] = product
            else:
                total[...] += product
        turned = total[...].T
        parts[far] = turned[: 2 * rows].reshape(2, rows, bottleneck)
        parts[near] = turned[2 * rows :].reshape(2, rows, bottleneck)

    def give(line, column, k):
        send(
            parts.at[line, column],
            parts_all.at[p],
            part_send.at[k],
            part_recv.at[p],
            {"proto_0": column, "proto_1": line},
        )

    for step in range(NZ // 2):
        far, near = at(4 + step), at(3 - step)
        back_of(far, near)
        give(far, a, 4 * step)
        give(far, b, 4 * step + 1)
        if step < NZ // 2 - 1:
            give(near, a, 4 * step + 2)
        give(near, b, 4 * step + 3)

    back = parts[z, a]
    for k in range(1, PEERS):
        peer = (p + k) % PEERS
        arrived(parts_all.at[peer], part_recv.at[peer])
        back = back + parts_all[peer]

    unit = unit_ref[...]
    inner = jnp.sum(unit * back, axis=1, keepdims=True)
    direction = ((back - unit * inner) / radius_ref[:, :1]).astype(BF16)
    dirs[d] = direction

    pair_core = d + 1 - 2 * (d % 2)
    for k in range(1, DP // 2):
        send(
            dirs.at[d], dirs.at[d], dir_send.at[k], dir_recv.at[d], {"dp": (d + 2 * k) % DP}
        )
    send(dirs.at[d], dirs.at[d], dir_send.at[0], dir_recv.at[d], {"dp": pair_core})
    for k in range(1, DP):
        peer, device = dp_peer(k)
        send(losses.at[d], losses.at[d], loss_send.at[k], loss_recv.at[d], device)

    hidden_out[...] = contract(direction, weight[...], ((1,), (1,))).astype(BF16)

    for k in range(1, DP // 2):
        peer = (d + 2 * k) % DP
        arrived(dirs.at[peer], dir_recv.at[peer])
        send(
            dirs.at[peer], dirs.at[peer], pass_send.at[k], dir_recv.at[peer], {"dp": pair_core}
        )
    for k in range(1, DP):
        peer = (d + k) % DP
        arrived(losses.at[peer], loss_recv.at[peer])
        arrived(picked_all.at[peer], pick_recv.at[peer])
    losses_p[p] = jnp.sum(losses[...], axis=0)
    for k in range(1, PEERS):
        peer, device = proto_peer(k)
        send(losses_p.at[p], losses_p.at[p], lossp_send.at[k], lossp_recv.at[p], device)
    for k in range(DP // 2):
        peer = (pair_core + 2 * k) % DP
        arrived(dirs.at[peer], dir_recv.at[peer])

    share_rows = heads.shape[1]
    product = contract(
        picked_all[...].reshape(DP * rows, share),
        dirs[...].reshape(DP * rows, bottleneck),
        ((0,), (0,)),
    )
    heads[...] = product.reshape(PEERS, share_rows, bottleneck)
    for k in range(1, PEERS):
        peer, device = proto_peer(k)
        send(heads.at[peer], heads_all.at[p], head_send.at[k], head_recv.at[p], device)
    result = heads[p]
    loss = losses_p[p]
    for k in range(1, PEERS):
        peer = (p + k) % PEERS
        arrived(losses_p.at[peer], lossp_recv.at[peer])
        loss = loss + losses_p[peer]
        arrived(heads_all.at[peer], head_recv.at[peer])
        result = result + heads_all[peer]
    head_out[...] = result
    loss = jnp.sum(jnp.sum(loss, axis=0, keepdims=True), axis=1, keepdims=True)
    loss_out[...] = loss / total_rows

    for copy in pending:
        copy.wait_send()


def per_device(hidden_states, teacher_feats, masks, head_weight, prototypes, center):
    images, patches, width = hidden_states.shape
    bottleneck = head_weight.shape[1]
    table = prototypes.shape[0]
    rows = masks.shape[0] * masks.shape[1]
    share = width // DP
    dma = pltpu.SemaphoreType.DMA
    scratch = [
        pltpu.VMEM(hidden_states.shape, BF16),
        pltpu.VMEM(teacher_feats.shape, BF16),
        pltpu.VMEM(head_weight.shape, BF16),
        pltpu.VMEM(prototypes.shape, BF16),
        pltpu.VMEM((table // 256, bottleneck, 256), BF16),
        pltpu.VMEM((table // 8, 8, 128), F32),
        pltpu.VMEM((NZ, 4, rows, bottleneck), BF16),
        pltpu.VMEM((NZ, table // 8, 8, 128), F32),
        pltpu.VMEM((NZ, table // 8, 8, 128), F32),
        pltpu.VMEM((rows, bottleneck), F32),
        pltpu.VMEM((rows, 128), F32),
        pltpu.VMEM((DP, rows, share), BF16),
        pltpu.VMEM((DP, rows, share), BF16),
        pltpu.VMEM((2, 8, 128), F32),
        pltpu.VMEM((PEERS, 2, 8, 128), F32),
        pltpu.VMEM((3, 8, 128), F32),
        pltpu.VMEM((table // KTILE, KTILE, 256), BF16),
        pltpu.VMEM((bottleneck, 256), F32),
        pltpu.VMEM((NZ, 2, rows, bottleneck), F32),
        pltpu.VMEM((PEERS, rows, bottleneck), F32),
        pltpu.VMEM((DP, rows, bottleneck), BF16),
        pltpu.VMEM((DP, 8, 128), F32),
        pltpu.VMEM((PEERS, 8, 128), F32),
        pltpu.VMEM((PEERS, share // PEERS, bottleneck), F32),
        pltpu.VMEM((PEERS, share // PEERS, bottleneck), F32),
        dma((4,)),
        dma((32,)),
        dma((NZ, 4)),
        dma((DP,)),
        dma((DP,)),
        dma((PEERS,)),
        dma((PEERS,)),
        dma((PEERS,)),
        dma((PEERS,)),
        dma((DP // 2,)),
        dma((DP,)),
        dma((DP // 2,)),
        dma((DP,)),
        dma((DP,)),
        dma((PEERS,)),
        dma((PEERS,)),
        dma((PEERS,)),
        dma((PEERS,)),
    ]
    vmem = pl.BlockSpec(memory_space=pltpu.VMEM)
    anywhere = pl.BlockSpec(memory_space=pl.ANY)
    loss, grad_hidden, grad_head = pl.pallas_call(
        kernel,
        out_shape=(
            jax.ShapeDtypeStruct((1, 1), F32),
            jax.ShapeDtypeStruct((rows, width), BF16),
            jax.ShapeDtypeStruct((share // PEERS, bottleneck), F32),
        ),
        in_specs=[vmem, anywhere, anywhere, anywhere, anywhere, vmem],
        out_specs=(vmem, vmem, vmem),
        scratch_shapes=scratch,
        compiler_params=pltpu.CompilerParams(
            collective_id=0, has_side_effects=True, vmem_limit_bytes=60 * 1024 * 1024
        ),
        name="ibot",
    )(
        masks,
        hidden_states,
        teacher_feats,
        head_weight,
        prototypes,
        center.reshape(-1, 128),
    )
    return (loss.reshape(()), grad_hidden, grad_head)


def solution(mesh):
    finer = Mesh(mesh.devices.reshape(DP, NX, NZ), DP_PROTO)
    placed = (
        P(DP_PROTO, None, None),
        P(DP_PROTO, None, None),
        P(DP_PROTO, None),
        P(),
        P(PROTO, None),
        P(PROTO),
    )
    return jax.shard_map(
        per_device,
        mesh=finer,
        in_specs=placed,
        out_specs=(P(), P(DP_PROTO, None), P(DP_PROTO, None)),
        check_vma=False,
    )
```

```python
import math

import jax
import jax.numpy as jnp
from jax import lax
from jax.experimental import pallas as pl
from jax.experimental.pallas import tpu as pltpu
from jax.sharding import Mesh
from jax.sharding import PartitionSpec as P

PROTO = ("proto_0", "proto_1")
DP_PROTO = ("dp", "proto_0", "proto_1")

STUDENT_TEMP = 0.1
TEACHER_TEMP = 0.07
LOSS_SCALE = 524288.0
EPSILON = 1e-06

LOG2E = 1.4426950408889634
LN2 = 0.6931471805599453
S_FACTOR = LOG2E / STUDENT_TEMP
T_FACTOR = LOG2E / TEACHER_TEMP

F32 = jnp.float32
BF16 = jnp.bfloat16
MESH = pl.DeviceIdType.MESH

DP = 16
NX = 2
NZ = 8
PEERS = NX * NZ
TILE = 1536
KTILE = 1024


def contract(left, right, dims):
    return lax.dot_general(left, right, (dims, ((), ())), preferred_element_type=F32)


def kernel(
    masks,
    hidden_hbm,
    teacher_hbm,
    weight_hbm,
    protos_hbm,
    center,
    loss_out,
    hidden_out,
    head_out,
    hidden,
    feats,
    weight,
    protos,
    protos_t,
    centers,
    rows_all,
    s_even,
    s_odd,
    t_even,
    t_odd,
    unit_ref,
    radius_ref,
    picked_mine,
    picked_all,
    stats,
    stats_all,
    top,
    grads,
    total,
    parts,
    side_in,
    up_in,
    down_in,
    dirs,
    losses,
    losses_p,
    heads,
    heads_all,
    load_sem,
    row_send,
    row_recv,
    pick_send,
    pick_recv,
    stat_send,
    stat_recv,
    side_send,
    side_recv,
    up_send,
    up_recv,
    down_send,
    down_recv,
    dir_send,
    dir_recv,
    pass_send,
    loss_send,
    loss_recv,
    lossp_send,
    lossp_recv,
    head_send,
    head_recv,
):
    d = lax.axis_index("dp")
    a = lax.axis_index("proto_0")
    z = lax.axis_index("proto_1")
    b = 1 - a
    p = a * NZ + z
    images, patches, _ = hidden.shape
    picks = masks.shape[1]
    rows = images * picks
    bottleneck = weight.shape[1]
    table = protos.shape[0]
    tiles = table // TILE
    lines = TILE // 8
    pending = []

    def send(src, dst, send_sem, recv_sem, device):
        copy = pltpu.make_async_remote_copy(
            src_ref=src,
            dst_ref=dst,
            send_sem=send_sem,
            recv_sem=recv_sem,
            device_id=device,
            device_id_type=MESH,
        )
        copy.start()
        pending.append(copy)

    def arrived(ref, sem):
        pltpu.make_async_remote_copy(
            src_ref=ref,
            dst_ref=ref,
            send_sem=sem,
            recv_sem=sem,
            device_id={"proto_0": b},
            device_id_type=MESH,
        ).wait_recv()

    def proto_peer(k):
        peer = (p + k) % PEERS
        return peer, {"proto_0": peer // NZ, "proto_1": peer % NZ}

    def dp_peer(k):
        peer = (d + k) % DP
        return peer, {"dp": peer}

    loads = [
        pltpu.make_async_copy(src, dst, load_sem.at[k])
        for k, (src, dst) in enumerate(
            (
                (hidden_hbm, hidden),
                (weight_hbm, weight),
                (teacher_hbm, feats),
                (protos_hbm, protos),
            )
        )
    ]
    for load in loads:
        load.start()

    barrier = pltpu.get_barrier_semaphore()
    for k in range(1, PEERS):
        pl.semaphore_signal(barrier, inc=1, device_id=proto_peer(k)[1], device_id_type=MESH)
    for k in range(1, DP):
        pl.semaphore_signal(barrier, inc=1, device_id=dp_peer(k)[1], device_id_type=MESH)

    loads[0].wait()
    loads[1].wait()
    loads[2].wait()
    picked_parts = []
    teacher_parts = []
    for image in range(images):
        index = lax.broadcasted_iota(jnp.int32, (patches, picks), 0)
        hot = (index == masks[image : image + 1, :]).astype(F32).astype(BF16)
        picked_parts.append(contract(hot, hidden[image], ((0,), (0,))).astype(BF16))
        teacher_parts.append(contract(hot, feats[image], ((0,), (0,))))
    picked = jnp.concatenate(picked_parts, axis=0)
    chosen = jnp.concatenate(teacher_parts, axis=0)
    raw = contract(picked, weight[...], ((1,), (0,)))
    radius = jnp.sqrt(jnp.sum(raw * raw, axis=1, keepdims=True) + EPSILON)
    unit = raw / radius
    unit_ref[...] = unit
    radius_ref[...] = jnp.broadcast_to(radius, radius_ref.shape)
    length = jnp.sqrt(jnp.sum(chosen * chosen, axis=1, keepdims=True) + EPSILON)
    rows_all[z, a] = unit.astype(BF16)
    rows_all[z, 2 + a] = (chosen / length).astype(BF16)
    share = picked_mine.shape[2]
    for k in range(DP):
        picked_mine[k] = picked[:, k * share : (k + 1) * share]

    loads[3].wait()
    for index in range(table // 256):
        protos_t[index] = protos[index * 256 : (index + 1) * 256, :].T
    for index in range(table // 128):
        column = jnp.broadcast_to(center[index : index + 1, :], (128, 128)).T
        centers[index * 16 : (index + 1) * 16] = column.reshape(16, 8, 128)

    pl.semaphore_wait(barrier, PEERS + DP - 2)

    above = {"proto_1": (z + 1) % NZ}
    below = {"proto_1": (z + NZ - 1) % NZ}
    beside = {"proto_0": b}
    row_count = []

    def at(step):
        return (z + step) % NZ

    def slot(other, step, kind):
        return at(step % NZ), (b if other else a) + 2 * kind

    def row_pass(other, step, kind, device):
        line, column = slot(other, step, kind)
        ref = rows_all.at[line, column]
        send(ref, ref, row_send.at[len(row_count)], row_recv.at[line, column], device)
        row_count.append(0)

    def row_wait(other, step, kind):
        line, column = slot(other, step, kind)
        arrived(rows_all.at[line, column], row_recv.at[line, column])

    for kind in (0, 1):
        row_pass(0, 0, kind, above)
        row_pass(0, 0, kind, below)
        row_pass(0, 0, kind, beside)

    for k in range(1, DP):
        peer, device = dp_peer(k)
        send(picked_mine.at[peer], picked_all.at[d], pick_send.at[k], pick_recv.at[d], device)
    picked_all[d] = picked_mine[d]

    def down(ref):
        return jnp.broadcast_to(ref, (8, 128))

    order = (0, 1, 7, 2, 6, 3, 5, 4)

    def held(step):
        place = order.index(step)
        refs = (s_odd, t_odd) if place % 2 else (s_even, t_even)
        return tuple(ref.at[place // 2] for ref in refs)

    def logits_tile(index, step, state):
        peak_s, peak_t = state
        s_ref, t_ref = held(step)
        first = pl.multiple_of(index * TILE, TILE)
        tile = protos[pl.ds(first, TILE), :]
        both = contract(tile, rows_all[at(step)].reshape(4 * rows, bottleneck), ((1,), (1,)))
        at_line = pl.ds(index * lines, lines)
        s = both[:, : 2 * rows].reshape(lines, 8, 128)
        t = both[:, 2 * rows :].reshape(lines, 8, 128) - centers[at_line]
        s_ref[at_line] = s
        t_ref[at_line] = t
        return jnp.maximum(peak_s, jnp.max(s, axis=0)), jnp.maximum(peak_t, jnp.max(t, axis=0))

    def weights_tile(index, step, peaks, state):
        total_s, total_t, cross = state
        s_ref, t_ref = held(step)
        at_line = pl.ds(index * lines, lines)
        s = s_ref[at_line]
        power_s = jnp.exp2((s - peaks[0]) * S_FACTOR)
        power_t = jnp.exp2((t_ref[at_line] - peaks[1]) * T_FACTOR)
        s_ref[at_line] = power_s
        t_ref[at_line] = power_t
        return (
            total_s + jnp.sum(power_s, axis=0),
            total_t + jnp.sum(power_t, axis=0),
            cross + jnp.sum(power_t * s, axis=0),
        )

    lowest = (jnp.full((8, 128), -jnp.inf, F32),) * 2
    zeros = (jnp.zeros((8, 128), F32),) * 3

    def peaks_of(state):
        return tuple(down(jnp.max(part, axis=0, keepdims=True)) for part in state)

    def finish(step, peaks, state):
        total_s, total_t, cross = (jnp.sum(part, axis=0, keepdims=True) for part in state)
        here = pl.ds(at(step), 1)
        shift_s = peaks[0][:1] * S_FACTOR
        shift_t = peaks[1][:1] * T_FACTOR
        top[0, here, :] = shift_s
        top[1, here, :] = shift_t
        top[2, here, :] = cross / total_t
        stats[0, here, :] = shift_s + jnp.log(total_s) * LOG2E
        stats[1, here, :] = shift_t + jnp.log(total_t) * LOG2E

    def first_pair(line):
        return peaks_of(
            lax.fori_loop(0, tiles, lambda i, state: logits_tile(i, line, state), lowest)
        )

    def pair(line, before, peaks):
        def body(index, state):
            return (
                logits_tile(index, line, state[0]),
                weights_tile(index, before, peaks, state[1]),
            )

        new, sums = lax.fori_loop(0, tiles, body, (lowest, zeros))
        finish(before, peaks, sums)
        return peaks_of(new)

    def last_pair(before, peaks):
        sums = lax.fori_loop(
            0, tiles, lambda i, state: weights_tile(i, before, peaks, state), zeros
        )
        finish(before, peaks, sums)

    for kind in (0, 1):
        row_wait(0, 1, kind)
        row_pass(0, 1, kind, below)
        row_pass(0, 1, kind, beside)
        row_wait(0, -1, kind)
        row_pass(0, -1, kind, above)
        row_pass(0, -1, kind, beside)
    row_wait(1, 0, 0)
    row_wait(1, 0, 1)
    peaks = first_pair(0)
    for kind in (0, 1):
        row_wait(0, 2, kind)
        row_pass(0, 2, kind, below)
        row_pass(0, 2, kind, beside)
        row_wait(0, -2, kind)
        row_pass(0, -2, kind, above)
        row_pass(0, -2, kind, beside)
    row_wait(1, 1, 0)
    row_wait(1, 1, 1)
    peaks = pair(1, 0, peaks)
    row_wait(1, -1, 0)
    row_wait(1, -1, 1)
    peaks = pair(7, 1, peaks)
    for kind in (0, 1):
        row_wait(1, 2, kind)
        row_pass(1, 2, kind, below)
        row_wait(1, -2, kind)
        row_pass(1, -2, kind, above)
    row_wait(0, 3, 0)
    row_pass(0, 3, 0, below)
    row_wait(0, -3, 1)
    row_pass(0, -3, 1, above)
    peaks = pair(2, 7, peaks)
    row_wait(1, 3, 0)
    row_pass(1, 3, 0, below)
    row_wait(1, -3, 1)
    row_pass(1, -3, 1, above)
    peaks = pair(6, 2, peaks)
    row_wait(0, 3, 1)
    row_wait(1, 3, 1)
    peaks = pair(3, 6, peaks)
    row_wait(0, -3, 0)
    row_wait(1, -3, 0)
    peaks = pair(5, 3, peaks)
    for kind in (0, 1):
        row_wait(0, 4, kind)
        row_wait(1, 4, kind)
    peaks = pair(4, 5, peaks)
    last_pair(4, peaks)

    for k in range(1, PEERS):
        peer, device = proto_peer(k)
        send(stats, stats_all.at[p], stat_send.at[k], stat_recv.at[p], device)
    stats_all[p] = stats[...]
    for k in range(1, PEERS):
        peer = (p + k) % PEERS
        arrived(stats_all.at[peer], stat_recv.at[peer])
    every = stats_all[...]
    highest = jnp.max(every, axis=0)
    joined = highest + jnp.log(jnp.sum(jnp.exp2(every - highest), axis=0)) * LOG2E
    total_rows = rows * PEERS * DP
    factor = math.log2(LOSS_SCALE / (total_rows * STUDENT_TEMP))
    losses[d] = joined[0] * (LN2 / PEERS) - top[2] * jnp.exp2(stats[1] - joined[1]) / STUDENT_TEMP
    top[0] = jnp.exp2(top[0] - joined[0] + factor)
    top[1] = jnp.exp2(top[1] - joined[1] + factor)

    def part_of(step, chunk):
        s_ref, t_ref = held(step)
        here = pl.ds(chunk * (KTILE // 8), KTILE // 8)
        up = down(top[0, pl.ds(at(step), 1), :])
        off = down(top[1, pl.ds(at(step), 1), :])
        value = s_ref[here] * up - t_ref[here] * off
        return value.reshape(KTILE, 128).astype(BF16)

    def back_of(far, near):
        for chunk in range(table // KTILE):
            grads[chunk, :, :128] = part_of(far, chunk)
            grads[chunk, :, 128:] = part_of(near, chunk)
        for chunk in range(table // KTILE):
            left = jnp.concatenate(
                [protos_t[chunk * (KTILE // 256) + k] for k in range(KTILE // 256)], axis=1
            )
            product = contract(left, grads[chunk], ((1,), (0,)))
            if chunk == 0:
                total[...] = product
            else:
                total[...] += product
        turned = total[...].T
        parts[far] = turned[: 2 * rows].reshape(2, rows, bottleneck)
        parts[near] = turned[2 * rows :].reshape(2, rows, bottleneck)

    half = rows // 2
    for step in range(NZ // 2):
        far, near = 4 + step, 3 - step
        back_of(far, near)
        for k in (far, near):
            send(parts.at[k, b], side_in.at[k], side_send.at[k], side_recv.at[k], beside)

    def gather_side(k):
        arrived(side_in.at[k], side_recv.at[k])
        parts[k, a] += side_in[k]

    first_half, second_half = pl.ds(0, half), pl.ds(half, half)
    gather_side(4)
    send(
        parts.at[4, a, first_half],
        up_in.at[3, first_half],
        up_send.at[3],
        up_recv.at[3],
        above,
    )
    send(
        parts.at[4, a, second_half],
        down_in.at[3, second_half],
        down_send.at[3],
        down_recv.at[3],
        below,
    )
    for k in (3, 2, 1):
        part = first_half if k == 3 else pl.ds(0, rows)
        gather_side(k)
        arrived(up_in.at[k, part], up_recv.at[k])
        parts[k, a, part] += up_in[k, part]
        send(parts.at[k, a], up_in.at[k - 1], up_send.at[k - 1], up_recv.at[k - 1], above)
        part = second_half if k == 3 else pl.ds(0, rows)
        gather_side(NZ - k)
        arrived(down_in.at[k, part], down_recv.at[k])
        parts[NZ - k, a, part] += down_in[k, part]
        send(
            parts.at[NZ - k, a],
            down_in.at[k - 1],
            down_send.at[k - 1],
            down_recv.at[k - 1],
            below,
        )
    arrived(side_in.at[0], side_recv.at[0])
    arrived(up_in.at[0], up_recv.at[0])
    arrived(down_in.at[0], down_recv.at[0])
    back = (parts[0, a] + side_in[0]) + (up_in[0] + down_in[0])

    unit = unit_ref[...]
    inner = jnp.sum(unit * back, axis=1, keepdims=True)
    direction = ((back - unit * inner) / radius_ref[:, :1]).astype(BF16)
    dirs[d] = direction

    pair_core = d + 1 - 2 * (d % 2)
    for k in range(1, DP // 2):
        send(
            dirs.at[d], dirs.at[d], dir_send.at[k], dir_recv.at[d], {"dp": (d + 2 * k) % DP}
        )
    send(dirs.at[d], dirs.at[d], dir_send.at[0], dir_recv.at[d], {"dp": pair_core})
    for k in range(1, DP):
        peer, device = dp_peer(k)
        send(losses.at[d], losses.at[d], loss_send.at[k], loss_recv.at[d], device)

    hidden_out[...] = contract(direction, weight[...], ((1,), (1,))).astype(BF16)

    for k in range(1, DP // 2):
        peer = (d + 2 * k) % DP
        arrived(dirs.at[peer], dir_recv.at[peer])
        send(
            dirs.at[peer], dirs.at[peer], pass_send.at[k], dir_recv.at[peer], {"dp": pair_core}
        )
    for k in range(1, DP):
        peer = (d + k) % DP
        arrived(losses.at[peer], loss_recv.at[peer])
        arrived(picked_all.at[peer], pick_recv.at[peer])
    losses_p[p] = jnp.sum(losses[...], axis=0)
    for k in range(1, PEERS):
        peer, device = proto_peer(k)
        send(losses_p.at[p], losses_p.at[p], lossp_send.at[k], lossp_recv.at[p], device)
    for k in range(DP // 2):
        peer = (pair_core + 2 * k) % DP
        arrived(dirs.at[peer], dir_recv.at[peer])

    share_rows = heads.shape[1]
    product = contract(
        picked_all[...].reshape(DP * rows, share),
        dirs[...].reshape(DP * rows, bottleneck),
        ((0,), (0,)),
    )
    heads[...] = product.reshape(PEERS, share_rows, bottleneck)
    for k in range(1, PEERS):
        peer, device = proto_peer(k)
        send(heads.at[peer], heads_all.at[p], head_send.at[k], head_recv.at[p], device)
    result = heads[p]
    loss = losses_p[p]
    for k in range(1, PEERS):
        peer = (p + k) % PEERS
        arrived(losses_p.at[peer], lossp_recv.at[peer])
        loss = loss + losses_p[peer]
        arrived(heads_all.at[peer], head_recv.at[peer])
        result = result + heads_all[peer]
    head_out[...] = result
    loss = jnp.sum(jnp.sum(loss, axis=0, keepdims=True), axis=1, keepdims=True)
    loss_out[...] = loss / total_rows

    for copy in pending:
        copy.wait_send()


def per_device(hidden_states, teacher_feats, masks, head_weight, prototypes, center):
    images, patches, width = hidden_states.shape
    bottleneck = head_weight.shape[1]
    table = prototypes.shape[0]
    rows = masks.shape[0] * masks.shape[1]
    share = width // DP
    dma = pltpu.SemaphoreType.DMA
    scratch = [
        pltpu.VMEM(hidden_states.shape, BF16),
        pltpu.VMEM(teacher_feats.shape, BF16),
        pltpu.VMEM(head_weight.shape, BF16),
        pltpu.VMEM(prototypes.shape, BF16),
        pltpu.VMEM((table // 256, bottleneck, 256), BF16),
        pltpu.VMEM((table // 8, 8, 128), F32),
        pltpu.VMEM((NZ, 4, rows, bottleneck), BF16),
        pltpu.VMEM((NZ // 2, table // 8, 8, 128), F32),
        pltpu.VMEM((NZ // 2, table // 8, 8, 128), F32),
        pltpu.VMEM((NZ // 2, table // 8, 8, 128), F32),
        pltpu.VMEM((NZ // 2, table // 8, 8, 128), F32),
        pltpu.VMEM((rows, bottleneck), F32),
        pltpu.VMEM((rows, 128), F32),
        pltpu.VMEM((DP, rows, share), BF16),
        pltpu.VMEM((DP, rows, share), BF16),
        pltpu.VMEM((2, 8, 128), F32),
        pltpu.VMEM((PEERS, 2, 8, 128), F32),
        pltpu.VMEM((3, 8, 128), F32),
        pltpu.VMEM((table // KTILE, KTILE, 256), BF16),
        pltpu.VMEM((bottleneck, 256), F32),
        pltpu.VMEM((NZ, 2, rows, bottleneck), F32),
        pltpu.VMEM((NZ, rows, bottleneck), F32),
        pltpu.VMEM((4, rows, bottleneck), F32),
        pltpu.VMEM((4, rows, bottleneck), F32),
        pltpu.VMEM((DP, rows, bottleneck), BF16),
        pltpu.VMEM((DP, 8, 128), F32),
        pltpu.VMEM((PEERS, 8, 128), F32),
        pltpu.VMEM((PEERS, share // PEERS, bottleneck), F32),
        pltpu.VMEM((PEERS, share // PEERS, bottleneck), F32),
        dma((4,)),
        dma((32,)),
        dma((NZ, 4)),
        dma((DP,)),
        dma((DP,)),
        dma((PEERS,)),
        dma((PEERS,)),
        dma((NZ,)),
        dma((NZ,)),
        dma((4,)),
        dma((4,)),
        dma((4,)),
        dma((4,)),
        dma((DP // 2,)),
        dma((DP,)),
        dma((DP // 2,)),
        dma((DP,)),
        dma((DP,)),
        dma((PEERS,)),
        dma((PEERS,)),
        dma((PEERS,)),
        dma((PEERS,)),
    ]
    vmem = pl.BlockSpec(memory_space=pltpu.VMEM)
    anywhere = pl.BlockSpec(memory_space=pl.ANY)
    loss, grad_hidden, grad_head = pl.pallas_call(
        kernel,
        out_shape=(
            jax.ShapeDtypeStruct((1, 1), F32),
            jax.ShapeDtypeStruct((rows, width), BF16),
            jax.ShapeDtypeStruct((share // PEERS, bottleneck), F32),
        ),
        in_specs=[vmem, anywhere, anywhere, anywhere, anywhere, vmem],
        out_specs=(vmem, vmem, vmem),
        scratch_shapes=scratch,
        compiler_params=pltpu.CompilerParams(
            collective_id=0, has_side_effects=True, vmem_limit_bytes=60 * 1024 * 1024
        ),
        name="ibot",
    )(
        masks,
        hidden_states,
        teacher_feats,
        head_weight,
        prototypes,
        center.reshape(-1, 128),
    )
    return (loss.reshape(()), grad_hidden, grad_head)


def solution(mesh):
    finer = Mesh(mesh.devices.reshape(DP, NX, NZ), DP_PROTO)
    placed = (
        P(DP_PROTO, None, None),
        P(DP_PROTO, None, None),
        P(DP_PROTO, None),
        P(),
        P(PROTO, None),
        P(PROTO),
    )
    return jax.shard_map(
        per_device,
        mesh=finer,
        in_specs=placed,
        out_specs=(P(), P(DP_PROTO, None), P(DP_PROTO, None)),
        check_vma=False,
    )
```

```python
import math

import jax
import jax.numpy as jnp
from jax import lax
from jax.experimental import pallas as pl
from jax.experimental.pallas import tpu as pltpu
from jax.sharding import Mesh
from jax.sharding import PartitionSpec as P

PROTO = ("proto_0", "proto_1")
DP_PROTO = ("dp", "proto_0", "proto_1")

STUDENT_TEMP = 0.1
TEACHER_TEMP = 0.07
LOSS_SCALE = 524288.0
EPSILON = 1e-06

LOG2E = 1.4426950408889634
LN2 = 0.6931471805599453
S_FACTOR = LOG2E / STUDENT_TEMP
T_FACTOR = LOG2E / TEACHER_TEMP

F32 = jnp.float32
BF16 = jnp.bfloat16
MESH = pl.DeviceIdType.MESH

DP = 16
NX = 2
NZ = 8
PEERS = NX * NZ
TILE = 1536
KTILE = 1024


def contract(left, right, dims):
    return lax.dot_general(left, right, (dims, ((), ())), preferred_element_type=F32)


def kernel(
    masks_hbm,
    hidden_hbm,
    teacher_hbm,
    weight_hbm,
    protos_hbm,
    center_hbm,
    loss_out,
    hidden_out,
    head_out,
    masks,
    center,
    hidden_rows,
    hidden,
    feats,
    weight,
    protos,
    protos_t,
    centers,
    rows_all,
    s_even,
    s_odd,
    t_even,
    t_odd,
    unit_ref,
    radius_ref,
    picked_mine,
    picked_all,
    stats,
    stats_all,
    top,
    grads,
    total,
    parts,
    side_in,
    up_in,
    down_in,
    up_other,
    down_other,
    dirs,
    losses,
    losses_p,
    heads,
    heads_all,
    load_sem,
    row_send,
    row_recv,
    pick_send,
    pick_recv,
    stat_send,
    stat_recv,
    side_send,
    side_recv,
    up_send,
    up_recv,
    down_send,
    down_recv,
    upo_send,
    upo_recv,
    downo_send,
    downo_recv,
    dir_send,
    dir_recv,
    pass_send,
    loss_send,
    loss_recv,
    lossp_send,
    lossp_recv,
    head_send,
    head_recv,
    ready,
):
    d = lax.axis_index("dp")
    a = lax.axis_index("proto_0")
    z = lax.axis_index("proto_1")
    b = 1 - a
    p = a * NZ + z
    images, patches, _ = hidden.shape
    picks = masks.shape[1]
    rows = images * picks
    bottleneck = weight.shape[1]
    table = protos.shape[0]
    tiles = table // TILE
    lines = TILE // 8
    pending = []

    def send(src, dst, send_sem, recv_sem, device):
        copy = pltpu.make_async_remote_copy(
            src_ref=src,
            dst_ref=dst,
            send_sem=send_sem,
            recv_sem=recv_sem,
            device_id=device,
            device_id_type=MESH,
        )
        copy.start()
        pending.append(copy)

    def arrived(ref, sem):
        pltpu.make_async_remote_copy(
            src_ref=ref,
            dst_ref=ref,
            send_sem=sem,
            recv_sem=sem,
            device_id={"proto_0": b},
            device_id_type=MESH,
        ).wait_recv()

    def proto_peer(k):
        peer = (p + k) % PEERS
        return peer, {"proto_0": peer // NZ, "proto_1": peer % NZ}

    def dp_peer(k):
        peer = (d + k) % DP
        return peer, {"dp": peer}

    barrier = pltpu.get_barrier_semaphore()
    above = {"proto_1": (z + 1) % NZ}
    below = {"proto_1": (z + NZ - 1) % NZ}
    beside = {"proto_0": b}
    partners = [{"dp": d + bit * (1 - 2 * ((d // bit) % 2))} for bit in (1, 2, 4, 8)]
    greeted = [above, below, beside, *partners]
    for device in greeted:
        pl.semaphore_signal(barrier, inc=1, device_id=device, device_id_type=MESH)

    loads = [
        pltpu.make_async_copy(src, dst, load_sem.at[k])
        for k, (src, dst) in enumerate(
            (
                (hidden_hbm, hidden),
                (weight_hbm, weight),
                (teacher_hbm, feats),
                (protos_hbm, protos),
                (masks_hbm, masks),
                (center_hbm, center),
            )
        )
    ]
    for load in (loads[4], *loads[:4], loads[5]):
        load.start()

    loads[4].wait()
    loads[0].wait()
    loads[1].wait()
    loads[2].wait()
    picked_parts = []
    teacher_parts = []
    for image in range(images):
        index = lax.broadcasted_iota(jnp.int32, (patches, picks), 0)
        hot = (index == masks[image : image + 1, :]).astype(F32).astype(BF16)
        picked_parts.append(contract(hot, hidden[image], ((0,), (0,))).astype(BF16))
        teacher_parts.append(contract(hot, feats[image], ((0,), (0,))))
    picked = jnp.concatenate(picked_parts, axis=0)
    chosen = jnp.concatenate(teacher_parts, axis=0)
    raw = contract(picked, weight[...], ((1,), (0,)))
    radius = jnp.sqrt(jnp.sum(raw * raw, axis=1, keepdims=True) + EPSILON)
    unit = raw / radius
    unit_ref[...] = unit
    radius_ref[...] = jnp.broadcast_to(radius, radius_ref.shape)
    length = jnp.sqrt(jnp.sum(chosen * chosen, axis=1, keepdims=True) + EPSILON)
    rows_all[z, a] = unit.astype(BF16)
    rows_all[z, 2 + a] = (chosen / length).astype(BF16)
    share = picked_mine.shape[2]
    for k in range(DP):
        picked_mine[k] = picked[:, k * share : (k + 1) * share]

    loads[3].wait()
    loads[5].wait()
    for index in range(table // 256):
        protos_t[index] = protos[index * 256 : (index + 1) * 256, :].T
    for index in range(table // 128):
        column = jnp.broadcast_to(center[index : index + 1, :], (128, 128)).T
        centers[index * 16 : (index + 1) * 16] = column.reshape(16, 8, 128)

    pl.semaphore_wait(barrier, len(greeted))

    above_two = {"proto_1": (z + 2) % NZ}
    below_two = {"proto_1": (z + NZ - 2) % NZ}
    row_count = []

    def at(step):
        return (z + step) % NZ

    small = rows // 2

    def slot(other, step, piece):
        kind, side = divmod(piece, 2)
        column = (b if other else a) + 2 * kind
        here = pl.ds(side * small, small)
        return rows_all.at[at(step % NZ), column, here], row_recv.at[at(step % NZ), column, side]

    def row_pass(other, step, piece, device):
        ref, sem = slot(other, step, piece)
        send(ref, ref, row_send.at[len(row_count)], sem, device)
        row_count.append(0)

    def row_wait(other, step, piece):
        ref, sem = slot(other, step, piece)
        arrived(ref, sem)

    every_piece = range(4)
    for piece in every_piece:
        row_pass(0, 0, piece, beside)
        row_pass(0, 0, piece, above)
        row_pass(0, 0, piece, below)

    def tell(turn):
        pl.semaphore_signal(
            ready.at[turn], inc=1, device_id=partners[turn], device_id_type=MESH
        )

    tell(0)
    def down(ref):
        return jnp.broadcast_to(ref, (8, 128))

    order = (0, 1, 7, 2, 6, 3, 5, 4)

    def held(step):
        place = order.index(step)
        refs = (s_odd, t_odd) if place % 2 else (s_even, t_even)
        return tuple(ref.at[place // 2] for ref in refs)

    def logits_tile(index, step, state):
        peak_s, peak_t = state
        s_ref, t_ref = held(step)
        first = pl.multiple_of(index * TILE, TILE)
        tile = protos[pl.ds(first, TILE), :]
        both = contract(tile, rows_all[at(step)].reshape(4 * rows, bottleneck), ((1,), (1,)))
        at_line = pl.ds(index * lines, lines)
        s = both[:, : 2 * rows].reshape(lines, 8, 128)
        t = both[:, 2 * rows :].reshape(lines, 8, 128) - centers[at_line]
        s_ref[at_line] = s
        t_ref[at_line] = t
        return jnp.maximum(peak_s, jnp.max(s, axis=0)), jnp.maximum(peak_t, jnp.max(t, axis=0))

    def weights_tile(index, step, peaks, state):
        total_s, total_t, cross = state
        s_ref, t_ref = held(step)
        at_line = pl.ds(index * lines, lines)
        s = s_ref[at_line]
        power_s = jnp.exp2((s - peaks[0]) * S_FACTOR)
        power_t = jnp.exp2((t_ref[at_line] - peaks[1]) * T_FACTOR)
        s_ref[at_line] = power_s
        t_ref[at_line] = power_t
        return (
            total_s + jnp.sum(power_s, axis=0),
            total_t + jnp.sum(power_t, axis=0),
            cross + jnp.sum(power_t * s, axis=0),
        )

    lowest = (jnp.full((8, 128), -jnp.inf, F32),) * 2
    zeros = (jnp.zeros((8, 128), F32),) * 3

    def peaks_of(state):
        return tuple(down(jnp.max(part, axis=0, keepdims=True)) for part in state)

    def finish(step, peaks, state):
        total_s, total_t, cross = (jnp.sum(part, axis=0, keepdims=True) for part in state)
        here = pl.ds(at(step), 1)
        shift_s = peaks[0][:1] * S_FACTOR
        shift_t = peaks[1][:1] * T_FACTOR
        top[0, here, :] = shift_s
        top[1, here, :] = shift_t
        top[2, here, :] = cross / total_t
        stats[0, here, :] = shift_s + jnp.log(total_s) * LOG2E
        stats[1, here, :] = shift_t + jnp.log(total_t) * LOG2E

    def first_pair(line):
        return peaks_of(
            lax.fori_loop(0, tiles, lambda i, state: logits_tile(i, line, state), lowest)
        )

    def pair(line, before, peaks):
        def body(index, state):
            return (
                logits_tile(index, line, state[0]),
                weights_tile(index, before, peaks, state[1]),
            )

        new, sums = lax.fori_loop(0, tiles, body, (lowest, zeros))
        finish(before, peaks, sums)
        return peaks_of(new)

    def last_pair(before, peaks):
        sums = lax.fori_loop(
            0, tiles, lambda i, state: weights_tile(i, before, peaks, state), zeros
        )
        finish(before, peaks, sums)

    for piece in every_piece:
        for step, device in ((1, below), (-1, above)):
            row_wait(0, step, piece)
            row_pass(0, step, piece, device)
            row_pass(0, step, piece, beside)
    for piece in every_piece:
        row_wait(1, 0, piece)
    pl.semaphore_wait(ready.at[0], 1)
    tell(1)
    peaks = first_pair(0)
    pl.semaphore_wait(ready.at[1], 1)
    tell(2)
    for piece in every_piece:
        for step, device in ((2, below), (-2, above)):
            row_wait(0, step, piece)
            row_pass(0, step, piece, device)
    for piece in every_piece:
        for step, device in ((1, below), (-1, above)):
            row_wait(1, step, piece)
            row_pass(1, step, piece, device)
    peaks = pair(1, 0, peaks)
    pl.semaphore_wait(ready.at[2], 1)
    for piece in every_piece:
        for step, device in ((3, below), (-3, above)):
            row_wait(0, step, piece)
            if (piece < 2) == (step > 0):
                row_pass(0, step, piece, device)
            row_pass(0, step, piece, beside)
    peaks = pair(7, 1, peaks)
    for piece in every_piece:
        row_wait(1, 2, piece)
    peaks = pair(2, 7, peaks)
    for piece in (0, 2, 1, 3):
        row_wait(0, 4, piece)
        row_pass(0, 4, piece, beside)
    for k in range(1, DP):
        peer, device = dp_peer(k)
        send(picked_mine.at[peer], picked_all.at[d], pick_send.at[k], pick_recv.at[d], device)
    picked_all[d] = picked_mine[d]
    for piece in every_piece:
        row_wait(1, -2, piece)
    peaks = pair(6, 2, peaks)
    for piece in every_piece:
        row_wait(1, 3, piece)
    peaks = pair(3, 6, peaks)
    for piece in every_piece:
        row_wait(1, -3, piece)
    peaks = pair(5, 3, peaks)
    for piece in every_piece:
        row_wait(1, 4, piece)
    peaks = pair(4, 5, peaks)
    last_pair(4, peaks)

    for k in range(1, PEERS):
        peer, device = proto_peer(k)
        send(stats, stats_all.at[p], stat_send.at[k], stat_recv.at[p], device)
    stats_all[p] = stats[...]
    for k in range(1, PEERS):
        peer = (p + k) % PEERS
        arrived(stats_all.at[peer], stat_recv.at[peer])
    every = stats_all[...]
    highest = jnp.max(every, axis=0)
    joined = highest + jnp.log(jnp.sum(jnp.exp2(every - highest), axis=0)) * LOG2E
    total_rows = rows * PEERS * DP
    factor = math.log2(LOSS_SCALE / (total_rows * STUDENT_TEMP))
    losses[d] = joined[0] * (LN2 / PEERS) - top[2] * jnp.exp2(stats[1] - joined[1]) / STUDENT_TEMP
    top[0] = jnp.exp2(top[0] - joined[0] + factor)
    top[1] = jnp.exp2(top[1] - joined[1] + factor)

    def part_of(step, chunk):
        s_ref, t_ref = held(step)
        here = pl.ds(chunk * (KTILE // 8), KTILE // 8)
        up = down(top[0, pl.ds(at(step), 1), :])
        off = down(top[1, pl.ds(at(step), 1), :])
        value = s_ref[here] * up - t_ref[here] * off
        return value.reshape(KTILE, 128).astype(BF16)

    def back_of(far, near):
        for chunk in range(table // KTILE):
            grads[chunk, :, :128] = part_of(far, chunk)
            grads[chunk, :, 128:] = part_of(near, chunk)
        for chunk in range(table // KTILE):
            left = jnp.concatenate(
                [protos_t[chunk * (KTILE // 256) + k] for k in range(KTILE // 256)], axis=1
            )
            product = contract(left, grads[chunk], ((1,), (0,)))
            if chunk == 0:
                total[...] = product
            else:
                total[...] += product
        turned = total[...].T
        parts[far] = turned[: 2 * rows].reshape(2, rows, bottleneck)
        parts[near] = turned[2 * rows :].reshape(2, rows, bottleneck)

    quarter = rows // 4

    def cut(piece):
        return pl.ds(piece * quarter, quarter)

    def give_side(step):
        for piece in every_piece:
            send(
                parts.at[step, b, cut(piece)],
                side_in.at[step, cut(piece)],
                side_send.at[step, piece],
                side_recv.at[step, piece],
                beside,
            )

    def give_along(column, step, piece, target, sems, device):
        send(
            parts.at[step, column, cut(piece)],
            target.at[cut(piece)],
            sems[0].at[piece],
            sems[1].at[piece],
            device,
        )

    def take(column, step, piece, source, sem):
        arrived(source.at[cut(piece)], sem.at[piece])
        parts[step, column, cut(piece)] += source[cut(piece)]

    def take_side(step, piece):
        take(a, step, piece, side_in.at[step], side_recv.at[step])

    def up(step, piece):
        k = step - 1
        device = above_two if step == 2 else above
        give_along(a, step, piece, up_in.at[k], (up_send.at[k], up_recv.at[k]), device)

    def low(step, piece):
        k = (-step) % NZ - 1
        device = below_two if step == 6 else below
        give_along(a, step, piece, down_in.at[k], (down_send.at[k], down_recv.at[k]), device)

    for step in range(NZ // 2):
        far, near = 4 + step, 3 - step
        back_of(far, near)
        for k in (far, near):
            if k in (4, 3, 5, 0):
                give_side(k)
        if near == 2:
            for piece in every_piece:
                give_along(b, 2, piece, up_other, (upo_send, upo_recv), above)
        if far == 6:
            for piece in every_piece:
                give_along(b, 6, piece, down_other, (downo_send, downo_recv), below)

    for piece in (0, 1):
        take_side(4, piece)
        up(4, piece)
    for piece in (2, 3):
        take_side(4, piece)
        low(4, piece)
    for piece in (2, 3):
        take_side(3, piece)
        up(3, piece)
        take_side(5, piece - 2)
        low(5, piece - 2)
    for piece in every_piece:
        take(b, 1, piece, up_other, upo_recv)
        take(b, 7, piece, down_other, downo_recv)
    give_side(1)
    give_side(7)
    for piece in (0, 1):
        take_side(3, piece)
        take(a, 3, piece, up_in.at[3], up_recv.at[3])
        up(3, piece)
        take_side(5, piece + 2)
        take(a, 5, piece + 2, down_in.at[3], down_recv.at[3])
        low(5, piece + 2)
    for piece in every_piece:
        turned_piece = (piece + 2) % 4
        take(a, 2, turned_piece, up_in.at[2], up_recv.at[2])
        up(2, turned_piece)
        take(a, 6, piece, down_in.at[2], down_recv.at[2])
        low(6, piece)
    for piece in every_piece:
        take_side(1, piece)
        up(1, piece)
        take_side(7, piece)
        low(7, piece)
    for piece in every_piece:
        take_side(0, piece)
        take(a, 0, piece, up_in.at[0], up_recv.at[0])
        take(a, 0, piece, down_in.at[0], down_recv.at[0])
        take(a, 0, piece, up_in.at[1], up_recv.at[1])
        take(a, 0, piece, down_in.at[1], down_recv.at[1])
    back = parts[0, a]

    unit = unit_ref[...]
    inner = jnp.sum(unit * back, axis=1, keepdims=True)
    direction = ((back - unit * inner) / radius_ref[:, :1]).astype(BF16)
    dirs[d] = direction

    pair_core = d + 1 - 2 * (d % 2)
    def chip_peer(y_step, x_step):
        return (d + 4 * y_step) % DP + 2 * x_step * (1 - 2 * ((d // 2) % 2))

    chips = ((2, 1), (1, 1), (3, 1), (0, 1), (2, 0), (1, 0), (3, 0))
    for k, steps in enumerate(chips):
        send(
            dirs.at[d], dirs.at[d], dir_send.at[k + 1], dir_recv.at[d], {"dp": chip_peer(*steps)}
        )
    send(dirs.at[d], dirs.at[d], dir_send.at[0], dir_recv.at[d], {"dp": pair_core})
    for k in range(1, DP):
        peer, device = dp_peer(k)
        send(losses.at[d], losses.at[d], loss_send.at[k], loss_recv.at[d], device)

    hidden_rows[...] = contract(direction, weight[...], ((1,), (1,))).astype(BF16)
    store = pltpu.make_async_copy(hidden_rows, hidden_out, load_sem.at[0])
    store.start()

    for k, steps in enumerate(chips[5:] + chips[4:5] + chips[:4]):
        peer = chip_peer(*steps)
        arrived(dirs.at[peer], dir_recv.at[peer])
        send(
            dirs.at[peer],
            dirs.at[peer],
            pass_send.at[k + 1],
            dir_recv.at[peer],
            {"dp": pair_core},
        )
    for k in range(1, DP):
        peer = (d + k) % DP
        arrived(losses.at[peer], loss_recv.at[peer])
        arrived(picked_all.at[peer], pick_recv.at[peer])
    losses_p[p] = jnp.sum(losses[...], axis=0)
    for k in range(1, PEERS):
        peer, device = proto_peer(k)
        send(losses_p.at[p], losses_p.at[p], lossp_send.at[k], lossp_recv.at[p], device)
    for k in range(DP // 2):
        peer = (pair_core + 2 * k) % DP
        arrived(dirs.at[peer], dir_recv.at[peer])

    share_rows = heads.shape[1]
    product = contract(
        picked_all[...].reshape(DP * rows, share),
        dirs[...].reshape(DP * rows, bottleneck),
        ((0,), (0,)),
    )
    heads[...] = product.reshape(PEERS, share_rows, bottleneck)
    for k in range(1, PEERS):
        peer, device = proto_peer(k)
        send(heads.at[peer], heads_all.at[p], head_send.at[k], head_recv.at[p], device)
    result = heads[p]
    loss = losses_p[p]
    for k in range(1, PEERS):
        peer = (p + k) % PEERS
        arrived(losses_p.at[peer], lossp_recv.at[peer])
        loss = loss + losses_p[peer]
        arrived(heads_all.at[peer], head_recv.at[peer])
        result = result + heads_all[peer]
    head_out[...] = result
    loss = jnp.sum(jnp.sum(loss, axis=0, keepdims=True), axis=1, keepdims=True)
    loss_out[...] = loss / total_rows

    store.wait()
    for copy in pending:
        copy.wait_send()


def per_device(hidden_states, teacher_feats, masks, head_weight, prototypes, center):
    images, patches, width = hidden_states.shape
    bottleneck = head_weight.shape[1]
    table = prototypes.shape[0]
    rows = masks.shape[0] * masks.shape[1]
    share = width // DP
    dma = pltpu.SemaphoreType.DMA
    scratch = [
        pltpu.VMEM(masks.shape, jnp.int32),
        pltpu.VMEM((table // 128, 128), F32),
        pltpu.VMEM((rows, width), BF16),
        pltpu.VMEM(hidden_states.shape, BF16),
        pltpu.VMEM(teacher_feats.shape, BF16),
        pltpu.VMEM(head_weight.shape, BF16),
        pltpu.VMEM(prototypes.shape, BF16),
        pltpu.VMEM((table // 256, bottleneck, 256), BF16),
        pltpu.VMEM((table // 8, 8, 128), F32),
        pltpu.VMEM((NZ, 4, rows, bottleneck), BF16),
        pltpu.VMEM((NZ // 2, table // 8, 8, 128), F32),
        pltpu.VMEM((NZ // 2, table // 8, 8, 128), F32),
        pltpu.VMEM((NZ // 2, table // 8, 8, 128), F32),
        pltpu.VMEM((NZ // 2, table // 8, 8, 128), F32),
        pltpu.VMEM((rows, bottleneck), F32),
        pltpu.VMEM((rows, 128), F32),
        pltpu.VMEM((DP, rows, share), BF16),
        pltpu.VMEM((DP, rows, share), BF16),
        pltpu.VMEM((2, 8, 128), F32),
        pltpu.VMEM((PEERS, 2, 8, 128), F32),
        pltpu.VMEM((3, 8, 128), F32),
        pltpu.VMEM((table // KTILE, KTILE, 256), BF16),
        pltpu.VMEM((bottleneck, 256), F32),
        pltpu.VMEM((NZ, 2, rows, bottleneck), F32),
        pltpu.VMEM((NZ, rows, bottleneck), F32),
        pltpu.VMEM((4, rows, bottleneck), F32),
        pltpu.VMEM((4, rows, bottleneck), F32),
        pltpu.VMEM((rows, bottleneck), F32),
        pltpu.VMEM((rows, bottleneck), F32),
        pltpu.VMEM((DP, rows, bottleneck), BF16),
        pltpu.VMEM((DP, 8, 128), F32),
        pltpu.VMEM((PEERS, 8, 128), F32),
        pltpu.VMEM((PEERS, share // PEERS, bottleneck), F32),
        pltpu.VMEM((PEERS, share // PEERS, bottleneck), F32),
        dma((6,)),
        dma((64,)),
        dma((NZ, 4, 2)),
        dma((DP,)),
        dma((DP,)),
        dma((PEERS,)),
        dma((PEERS,)),
        dma((NZ, 4)),
        dma((NZ, 4)),
        dma((4, 4)),
        dma((4, 4)),
        dma((4, 4)),
        dma((4, 4)),
        dma((4,)),
        dma((4,)),
        dma((4,)),
        dma((4,)),
        dma((DP // 2,)),
        dma((DP,)),
        dma((DP // 2,)),
        dma((DP,)),
        dma((DP,)),
        dma((PEERS,)),
        dma((PEERS,)),
        dma((PEERS,)),
        dma((PEERS,)),
        pltpu.SemaphoreType.REGULAR((3,)),
    ]
    vmem = pl.BlockSpec(memory_space=pltpu.VMEM)
    anywhere = pl.BlockSpec(memory_space=pl.ANY)
    loss, grad_hidden, grad_head = pl.pallas_call(
        kernel,
        out_shape=(
            jax.ShapeDtypeStruct((1, 1), F32),
            jax.ShapeDtypeStruct((rows, width), BF16),
            jax.ShapeDtypeStruct((share // PEERS, bottleneck), F32),
        ),
        in_specs=[anywhere] * 6,
        out_specs=(vmem, anywhere, vmem),
        scratch_shapes=scratch,
        compiler_params=pltpu.CompilerParams(
            collective_id=0, has_side_effects=True, vmem_limit_bytes=60 * 1024 * 1024
        ),
        name="ibot",
    )(
        masks,
        hidden_states,
        teacher_feats,
        head_weight,
        prototypes,
        center.reshape(-1, 128),
    )
    def hand(*refs):
        for source, target in zip(refs[:3], refs[3:]):
            target[...] = source[...]

    loss, grad_hidden, grad_head = pl.pallas_call(
        hand,
        out_shape=tuple(
            jax.ShapeDtypeStruct(part.shape, part.dtype) for part in (loss, grad_hidden, grad_head)
        ),
        name="hand",
    )(loss, grad_hidden, grad_head)
    return (loss.reshape(()), grad_hidden, grad_head)


def solution(mesh):
    finer = Mesh(mesh.devices.reshape(DP, NX, NZ), DP_PROTO)
    placed = (
        P(DP_PROTO, None, None),
        P(DP_PROTO, None, None),
        P(DP_PROTO, None),
        P(),
        P(PROTO, None),
        P(PROTO),
    )
    return jax.shard_map(
        per_device,
        mesh=finer,
        in_specs=placed,
        out_specs=(P(), P(DP_PROTO, None), P(DP_PROTO, None)),
        check_vma=False,
    )
```

```python
import math

import jax
import jax.numpy as jnp
from jax import lax
from jax.experimental import pallas as pl
from jax.experimental.pallas import tpu as pltpu
from jax.sharding import Mesh
from jax.sharding import PartitionSpec as P

PROTO = ("proto_0", "proto_1")
DP_PROTO = ("dp", "proto_0", "proto_1")

STUDENT_TEMP = 0.1
TEACHER_TEMP = 0.07
LOSS_SCALE = 524288.0
EPSILON = 1e-06

LOG2E = 1.4426950408889634
LN2 = 0.6931471805599453
S_FACTOR = LOG2E / STUDENT_TEMP
T_FACTOR = LOG2E / TEACHER_TEMP

F32 = jnp.float32
BF16 = jnp.bfloat16
MESH = pl.DeviceIdType.MESH

DP = 16
NX = 2
NZ = 8
PEERS = NX * NZ
TILE = 1536
PART = 256
KTILE = 256


def contract(left, right, dims):
    return lax.dot_general(left, right, (dims, ((), ())), preferred_element_type=F32)


def kernel(
    masks_hbm,
    hidden_hbm,
    teacher_hbm,
    weight_hbm,
    protos_hbm,
    center_hbm,
    loss_out,
    hidden_out,
    head_out,
    masks,
    center,
    hidden_rows,
    hidden,
    feats,
    weight,
    protos,
    protos_t,
    centers,
    rows_all,
    s_even,
    s_odd,
    t_even,
    t_odd,
    unit_ref,
    radius_ref,
    picked_mine,
    picked_all,
    stats,
    stats_all,
    top,
    parts,
    side_in,
    up_in,
    down_in,
    up_other,
    down_other,
    dirs,
    losses,
    losses_p,
    heads,
    heads_all,
    heads_full,
    load_sem,
    row_send,
    row_recv,
    pick_send,
    pick_recv,
    stat_send,
    stat_recv,
    side_send,
    side_recv,
    up_send,
    up_recv,
    down_send,
    down_recv,
    upo_send,
    upo_recv,
    downo_send,
    downo_recv,
    dir_send,
    dir_recv,
    pass_send,
    loss_send,
    loss_recv,
    lossp_send,
    lossp_recv,
    head_send,
    head_recv,
    ready,
):
    d = lax.axis_index("dp")
    a = lax.axis_index("proto_0")
    z = lax.axis_index("proto_1")
    b = 1 - a
    p = a * NZ + z
    images, patches, _ = hidden.shape
    picks = masks.shape[1]
    rows = images * picks
    bottleneck = weight.shape[1]
    table = protos.shape[0]
    tiles = table // TILE
    lines = PART // 8
    cuts = TILE // PART
    pending = []

    def send(src, dst, send_sem, recv_sem, device):
        copy = pltpu.make_async_remote_copy(
            src_ref=src,
            dst_ref=dst,
            send_sem=send_sem,
            recv_sem=recv_sem,
            device_id=device,
            device_id_type=MESH,
        )
        copy.start()
        pending.append(copy)

    def arrived(ref, sem):
        pltpu.make_async_remote_copy(
            src_ref=ref,
            dst_ref=ref,
            send_sem=sem,
            recv_sem=sem,
            device_id={"proto_0": b},
            device_id_type=MESH,
        ).wait_recv()

    def proto_peer(k):
        peer = (p + k) % PEERS
        return peer, {"proto_0": peer // NZ, "proto_1": peer % NZ}

    def dp_peer(k):
        peer = (d + k) % DP
        return peer, {"dp": peer}

    barrier = pltpu.get_barrier_semaphore()
    above = {"proto_1": (z + 1) % NZ}
    below = {"proto_1": (z + NZ - 1) % NZ}
    beside = {"proto_0": b}
    partners = [{"dp": d + bit * (1 - 2 * ((d // bit) % 2))} for bit in (1, 2, 4, 8)]
    greeted = [above, below, beside, *partners]
    for device in greeted:
        pl.semaphore_signal(barrier, inc=1, device_id=device, device_id_type=MESH)

    loads = [
        pltpu.make_async_copy(src, dst, load_sem.at[k])
        for k, (src, dst) in enumerate(
            (
                (hidden_hbm, hidden),
                (weight_hbm, weight),
                (teacher_hbm, feats),
                (protos_hbm, protos),
                (masks_hbm, masks),
                (center_hbm, center),
            )
        )
    ]
    for load in (loads[4], *loads[:4], loads[5]):
        load.start()

    loads[4].wait()
    loads[0].wait()
    loads[1].wait()
    loads[2].wait()
    picked_parts = []
    teacher_parts = []
    for image in range(images):
        index = lax.broadcasted_iota(jnp.int32, (patches, picks), 0)
        hot = (index == masks[image : image + 1, :]).astype(F32).astype(BF16)
        picked_parts.append(contract(hot, hidden[image], ((0,), (0,))).astype(BF16))
        teacher_parts.append(contract(hot, feats[image], ((0,), (0,))))
    picked = jnp.concatenate(picked_parts, axis=0)
    chosen = jnp.concatenate(teacher_parts, axis=0)
    raw = contract(picked, weight[...], ((1,), (0,)))
    radius = jnp.sqrt(jnp.sum(raw * raw, axis=1, keepdims=True) + EPSILON)
    unit = raw / radius
    unit_ref[...] = unit
    radius_ref[...] = jnp.broadcast_to(radius, radius_ref.shape)
    length = jnp.sqrt(jnp.sum(chosen * chosen, axis=1, keepdims=True) + EPSILON)
    rows_all[z, a] = unit.astype(BF16)
    rows_all[z, 2 + a] = (chosen / length).astype(BF16)
    share = picked_mine.shape[2]
    for k in range(DP):
        picked_mine[k] = picked[:, k * share : (k + 1) * share]

    loads[3].wait()
    loads[5].wait()
    for index in range(table // 256):
        protos_t[index] = protos[index * 256 : (index + 1) * 256, :].T
    for index in range(table // 128):
        column = jnp.broadcast_to(center[index : index + 1, :], (128, 128)).T
        centers[index * 16 : (index + 1) * 16] = column.reshape(16, 8, 128)

    pl.semaphore_wait(barrier, len(greeted))

    above_two = {"proto_1": (z + 2) % NZ}
    below_two = {"proto_1": (z + NZ - 2) % NZ}
    row_count = []

    def at(step):
        return (z + step) % NZ

    small = rows // 2

    def slot(other, step, piece):
        kind, side = divmod(piece, 2)
        column = (b if other else a) + 2 * kind
        here = pl.ds(side * small, small)
        return rows_all.at[at(step % NZ), column, here], row_recv.at[at(step % NZ), column, side]

    def row_pass(other, step, piece, device):
        ref, sem = slot(other, step, piece)
        send(ref, ref, row_send.at[len(row_count)], sem, device)
        row_count.append(0)

    def row_wait(other, step, piece):
        ref, sem = slot(other, step, piece)
        arrived(ref, sem)

    every_piece = range(4)
    for piece in every_piece:
        row_pass(0, 0, piece, beside)
        row_pass(0, 0, piece, above)
        row_pass(0, 0, piece, below)

    def tell(turn):
        pl.semaphore_signal(
            ready.at[turn], inc=1, device_id=partners[turn], device_id_type=MESH
        )

    tell(0)
    def down(ref):
        return jnp.broadcast_to(ref, (8, 128))

    order = (0, 1, 7, 2, 6, 3, 5, 4)

    def held(step):
        place = order.index(step)
        refs = (s_odd, t_odd) if place % 2 else (s_even, t_even)
        return tuple(ref.at[place // 2] for ref in refs)

    def logits_tile(index, step, state):
        peak_s, peak_t = state
        s_ref, t_ref = held(step)
        first = pl.multiple_of(index * PART, PART)
        tile = protos[pl.ds(first, PART), :]
        both = contract(tile, rows_all[at(step)].reshape(4 * rows, bottleneck), ((1,), (1,)))
        at_line = pl.ds(index * lines, lines)
        s = both[:, : 2 * rows].reshape(lines, 8, 128)
        t = both[:, 2 * rows :].reshape(lines, 8, 128) - centers[at_line]
        s_ref[at_line] = s
        t_ref[at_line] = t
        return jnp.maximum(peak_s, jnp.max(s, axis=0)), jnp.maximum(peak_t, jnp.max(t, axis=0))

    def weights_tile(index, step, peaks, state):
        total_s, total_t, cross = state
        s_ref, t_ref = held(step)
        at_line = pl.ds(index * lines, lines)
        s = s_ref[at_line]
        power_s = jnp.exp2((s - peaks[0]) * S_FACTOR)
        power_t = jnp.exp2((t_ref[at_line] - peaks[1]) * T_FACTOR)
        s_ref[at_line] = power_s
        t_ref[at_line] = power_t
        return (
            total_s + jnp.sum(power_s, axis=0),
            total_t + jnp.sum(power_t, axis=0),
            cross + jnp.sum(power_t * s, axis=0),
        )

    lowest = (jnp.full((8, 128), -jnp.inf, F32),) * 2
    zeros = (jnp.zeros((8, 128), F32),) * 3

    def peaks_of(state):
        return tuple(down(jnp.max(part, axis=0, keepdims=True)) for part in state)

    def finish(step, peaks, state):
        total_s, total_t, cross = (jnp.sum(part, axis=0, keepdims=True) for part in state)
        here = pl.ds(at(step), 1)
        shift_s = peaks[0][:1] * S_FACTOR
        shift_t = peaks[1][:1] * T_FACTOR
        top[0, here, :] = shift_s
        top[1, here, :] = shift_t
        top[2, here, :] = cross / total_t
        stats[0, here, :] = shift_s + jnp.log(total_s) * LOG2E
        stats[1, here, :] = shift_t + jnp.log(total_t) * LOG2E

    def many(index, state, work, *given):
        for k in range(cuts):
            state = work(index * cuts + k, *given, state)
        return state

    def first_pair(line):
        return peaks_of(
            lax.fori_loop(0, tiles, lambda i, state: many(i, state, logits_tile, line), lowest)
        )

    def pair(line, before, peaks):
        def body(index, state):
            new, sums = state
            for k in range(cuts):
                new = logits_tile(index * cuts + k, line, new)
                sums = weights_tile(index * cuts + k, before, peaks, sums)
            return new, sums

        new, sums = lax.fori_loop(0, tiles, body, (lowest, zeros))
        finish(before, peaks, sums)
        return peaks_of(new)

    def last_pair(before, peaks):
        sums = lax.fori_loop(
            0, tiles, lambda i, state: many(i, state, weights_tile, before, peaks), zeros
        )
        finish(before, peaks, sums)

    for piece in every_piece:
        for step, device in ((1, below), (-1, above)):
            row_wait(0, step, piece)
            row_pass(0, step, piece, device)
            row_pass(0, step, piece, beside)
    for piece in every_piece:
        row_wait(1, 0, piece)
    pl.semaphore_wait(ready.at[0], 1)
    tell(1)
    peaks = first_pair(0)
    pl.semaphore_wait(ready.at[1], 1)
    tell(2)
    for piece in every_piece:
        for step, device in ((2, below), (-2, above)):
            row_wait(0, step, piece)
            row_pass(0, step, piece, device)
    for piece in every_piece:
        for step, device in ((1, below), (-1, above)):
            row_wait(1, step, piece)
            row_pass(1, step, piece, device)
    peaks = pair(1, 0, peaks)
    pl.semaphore_wait(ready.at[2], 1)
    for piece in every_piece:
        for step, device in ((3, below), (-3, above)):
            row_wait(0, step, piece)
            if (piece < 2) == (step > 0):
                row_pass(0, step, piece, device)
            row_pass(0, step, piece, beside)
    peaks = pair(7, 1, peaks)
    for piece in every_piece:
        row_wait(1, 2, piece)
    peaks = pair(2, 7, peaks)
    for piece in (0, 2, 1, 3):
        row_wait(0, 4, piece)
        row_pass(0, 4, piece, beside)
    for piece in every_piece:
        row_wait(1, -2, piece)
    peaks = pair(6, 2, peaks)
    for piece in every_piece:
        row_wait(1, 3, piece)
    peaks = pair(3, 6, peaks)
    for piece in every_piece:
        row_wait(1, -3, piece)
    peaks = pair(5, 3, peaks)
    for piece in every_piece:
        row_wait(1, 4, piece)
    peaks = pair(4, 5, peaks)
    last_pair(4, peaks)

    for k in range(1, PEERS):
        peer, device = proto_peer(k)
        send(stats, stats_all.at[p], stat_send.at[k], stat_recv.at[p], device)
    for k in range(1, DP):
        peer, device = dp_peer(k)
        send(picked_mine.at[peer], picked_all.at[d], pick_send.at[k], pick_recv.at[d], device)
    picked_all[d] = picked_mine[d]
    stats_all[p] = stats[...]
    for k in range(1, PEERS):
        peer = (p + k) % PEERS
        arrived(stats_all.at[peer], stat_recv.at[peer])
    every = stats_all[...]
    highest = jnp.max(every, axis=0)
    joined = highest + jnp.log(jnp.sum(jnp.exp2(every - highest), axis=0)) * LOG2E
    total_rows = rows * PEERS * DP
    factor = math.log2(LOSS_SCALE / (total_rows * STUDENT_TEMP))
    losses[d] = joined[0] * (LN2 / PEERS) - top[2] * jnp.exp2(stats[1] - joined[1]) / STUDENT_TEMP
    top[0] = jnp.exp2(top[0] - joined[0] + factor)
    top[1] = jnp.exp2(top[1] - joined[1] + factor)

    def part_of(step, chunk):
        s_ref, t_ref = held(step)
        here = pl.ds(chunk * (KTILE // 8), KTILE // 8)
        up = down(top[0, pl.ds(at(step), 1), :])
        off = down(top[1, pl.ds(at(step), 1), :])
        value = s_ref[here] * up - t_ref[here] * off
        return value.reshape(KTILE, 128).astype(BF16)

    def back_of(far, near):
        product = None
        for chunk in range(table // KTILE):
            right = jnp.concatenate([part_of(far, chunk), part_of(near, chunk)], axis=1)
            left = jnp.concatenate(
                [protos_t[chunk * (KTILE // 256) + k] for k in range(KTILE // 256)], axis=1
            )
            piece = contract(left, right, ((1,), (0,)))
            product = piece if product is None else product + piece
        turned = product.T
        parts[far] = turned[: 2 * rows].reshape(2, rows, bottleneck)
        parts[near] = turned[2 * rows :].reshape(2, rows, bottleneck)

    quarter = rows // 4

    def cut(piece):
        return pl.ds(piece * quarter, quarter)

    def give_side(step):
        for piece in every_piece:
            send(
                parts.at[step, b, cut(piece)],
                side_in.at[step, cut(piece)],
                side_send.at[step, piece],
                side_recv.at[step, piece],
                beside,
            )

    def give_along(column, step, piece, target, sems, device):
        send(
            parts.at[step, column, cut(piece)],
            target.at[cut(piece)],
            sems[0].at[piece],
            sems[1].at[piece],
            device,
        )

    def take(column, step, piece, source, sem):
        arrived(source.at[cut(piece)], sem.at[piece])
        parts[step, column, cut(piece)] += source[cut(piece)]

    def take_side(step, piece):
        take(a, step, piece, side_in.at[step], side_recv.at[step])

    def up(step, piece):
        k = step - 1
        device = above_two if step == 2 else above
        give_along(a, step, piece, up_in.at[k], (up_send.at[k], up_recv.at[k]), device)

    def low(step, piece):
        k = (-step) % NZ - 1
        device = below_two if step == 6 else below
        give_along(a, step, piece, down_in.at[k], (down_send.at[k], down_recv.at[k]), device)

    back_of(4, 3)
    give_side(4)
    give_side(3)
    back_of(5, 2)
    give_side(5)
    for piece in every_piece:
        give_along(b, 2, piece, up_other, (upo_send, upo_recv), above)
    back_of(6, 1)
    for piece in every_piece:
        give_along(b, 6, piece, down_other, (downo_send, downo_recv), below)
    for piece in (0, 1):
        take_side(4, piece)
        up(4, piece)
    for piece in (2, 3):
        take_side(4, piece)
        low(4, piece)
    back_of(7, 0)
    give_side(0)
    for piece in (2, 3):
        take_side(3, piece)
        up(3, piece)
        take_side(5, piece - 2)
        low(5, piece - 2)
    for piece in every_piece:
        take(b, 1, piece, up_other, upo_recv)
        take(b, 7, piece, down_other, downo_recv)
    give_side(1)
    give_side(7)
    for piece in (0, 1):
        take_side(3, piece)
        take(a, 3, piece, up_in.at[3], up_recv.at[3])
        up(3, piece)
        take_side(5, piece + 2)
        take(a, 5, piece + 2, down_in.at[3], down_recv.at[3])
        low(5, piece + 2)
    for piece in every_piece:
        turned_piece = (piece + 2) % 4
        take(a, 2, turned_piece, up_in.at[2], up_recv.at[2])
        up(2, turned_piece)
        take(a, 6, piece, down_in.at[2], down_recv.at[2])
        low(6, piece)
    for piece in every_piece:
        take_side(1, piece)
        up(1, piece)
        take_side(7, piece)
        low(7, piece)
    for piece in every_piece:
        take_side(0, piece)
        take(a, 0, piece, up_in.at[0], up_recv.at[0])
        take(a, 0, piece, down_in.at[0], down_recv.at[0])
        take(a, 0, piece, up_in.at[1], up_recv.at[1])
        take(a, 0, piece, down_in.at[1], down_recv.at[1])
    back = parts[0, a]

    unit = unit_ref[...]
    inner = jnp.sum(unit * back, axis=1, keepdims=True)
    direction = ((back - unit * inner) / radius_ref[:, :1]).astype(BF16)
    dirs[d] = direction

    pair_core = d + 1 - 2 * (d % 2)
    def chip_peer(y_step, x_step):
        return (d + 4 * y_step) % DP + 2 * x_step * (1 - 2 * ((d // 2) % 2))

    chips = ((2, 1), (1, 1), (3, 1), (0, 1), (2, 0), (1, 0), (3, 0))
    for k, steps in enumerate(chips):
        send(
            dirs.at[d], dirs.at[d], dir_send.at[k + 1], dir_recv.at[d], {"dp": chip_peer(*steps)}
        )
    send(dirs.at[d], dirs.at[d], dir_send.at[0], dir_recv.at[d], {"dp": pair_core})
    for k in range(1, DP):
        peer, device = dp_peer(k)
        send(losses.at[d], losses.at[d], loss_send.at[k], loss_recv.at[d], device)

    hidden_rows[...] = contract(direction, weight[...], ((1,), (1,))).astype(BF16)
    store = pltpu.make_async_copy(hidden_rows, hidden_out, load_sem.at[0])
    store.start()

    for k, steps in enumerate(chips[5:] + chips[4:5] + chips[:4]):
        peer = chip_peer(*steps)
        arrived(dirs.at[peer], dir_recv.at[peer])
        send(
            dirs.at[peer],
            dirs.at[peer],
            pass_send.at[k + 1],
            dir_recv.at[peer],
            {"dp": pair_core},
        )
    for k in range(1, DP):
        peer = (d + k) % DP
        arrived(losses.at[peer], loss_recv.at[peer])
        arrived(picked_all.at[peer], pick_recv.at[peer])
    losses_p[p] = jnp.sum(losses[...], axis=0)
    for k in range(1, PEERS):
        peer, device = proto_peer(k)
        send(losses_p.at[p], losses_p.at[p], lossp_send.at[k], lossp_recv.at[p], device)
    for k in range(DP // 2):
        peer = (pair_core + 2 * k) % DP
        arrived(dirs.at[peer], dir_recv.at[peer])

    share_rows = heads.shape[1]
    product = contract(
        picked_all[...].reshape(DP * rows, share),
        dirs[...].reshape(DP * rows, bottleneck),
        ((0,), (0,)),
    )
    product = product.reshape(PEERS, share_rows, bottleneck)
    heads_full[...] = product
    heads[...] = product.astype(BF16)
    for k in range(1, PEERS):
        peer, device = proto_peer(k)
        send(heads.at[peer], heads_all.at[p], head_send.at[k], head_recv.at[p], device)
    result = heads_full[p]
    loss = losses_p[p]
    for k in range(1, PEERS):
        peer = (p + k) % PEERS
        arrived(losses_p.at[peer], lossp_recv.at[peer])
        loss = loss + losses_p[peer]
        arrived(heads_all.at[peer], head_recv.at[peer])
        result = result + heads_all[peer].astype(F32)
    head_out[...] = result
    loss = jnp.sum(jnp.sum(loss, axis=0, keepdims=True), axis=1, keepdims=True)
    loss_out[...] = loss / total_rows

    store.wait()
    for copy in pending:
        copy.wait_send()


def per_device(hidden_states, teacher_feats, masks, head_weight, prototypes, center):
    images, patches, width = hidden_states.shape
    bottleneck = head_weight.shape[1]
    table = prototypes.shape[0]
    rows = masks.shape[0] * masks.shape[1]
    share = width // DP
    dma = pltpu.SemaphoreType.DMA
    scratch = [
        pltpu.VMEM(masks.shape, jnp.int32),
        pltpu.VMEM((table // 128, 128), F32),
        pltpu.VMEM((rows, width), BF16),
        pltpu.VMEM(hidden_states.shape, BF16),
        pltpu.VMEM(teacher_feats.shape, BF16),
        pltpu.VMEM(head_weight.shape, BF16),
        pltpu.VMEM(prototypes.shape, BF16),
        pltpu.VMEM((table // 256, bottleneck, 256), BF16),
        pltpu.VMEM((table // 8, 8, 128), F32),
        pltpu.VMEM((NZ, 4, rows, bottleneck), BF16),
        pltpu.VMEM((NZ // 2, table // 8, 8, 128), F32),
        pltpu.VMEM((NZ // 2, table // 8, 8, 128), F32),
        pltpu.VMEM((NZ // 2, table // 8, 8, 128), F32),
        pltpu.VMEM((NZ // 2, table // 8, 8, 128), F32),
        pltpu.VMEM((rows, bottleneck), F32),
        pltpu.VMEM((rows, 128), F32),
        pltpu.VMEM((DP, rows, share), BF16),
        pltpu.VMEM((DP, rows, share), BF16),
        pltpu.VMEM((2, 8, 128), F32),
        pltpu.VMEM((PEERS, 2, 8, 128), F32),
        pltpu.VMEM((3, 8, 128), F32),
        pltpu.VMEM((NZ, 2, rows, bottleneck), F32),
        pltpu.VMEM((NZ, rows, bottleneck), F32),
        pltpu.VMEM((4, rows, bottleneck), F32),
        pltpu.VMEM((4, rows, bottleneck), F32),
        pltpu.VMEM((rows, bottleneck), F32),
        pltpu.VMEM((rows, bottleneck), F32),
        pltpu.VMEM((DP, rows, bottleneck), BF16),
        pltpu.VMEM((DP, 8, 128), F32),
        pltpu.VMEM((PEERS, 8, 128), F32),
        pltpu.VMEM((PEERS, share // PEERS, bottleneck), BF16),
        pltpu.VMEM((PEERS, share // PEERS, bottleneck), BF16),
        pltpu.VMEM((PEERS, share // PEERS, bottleneck), F32),
        dma((6,)),
        dma((64,)),
        dma((NZ, 4, 2)),
        dma((DP,)),
        dma((DP,)),
        dma((PEERS,)),
        dma((PEERS,)),
        dma((NZ, 4)),
        dma((NZ, 4)),
        dma((4, 4)),
        dma((4, 4)),
        dma((4, 4)),
        dma((4, 4)),
        dma((4,)),
        dma((4,)),
        dma((4,)),
        dma((4,)),
        dma((DP // 2,)),
        dma((DP,)),
        dma((DP // 2,)),
        dma((DP,)),
        dma((DP,)),
        dma((PEERS,)),
        dma((PEERS,)),
        dma((PEERS,)),
        dma((PEERS,)),
        pltpu.SemaphoreType.REGULAR((3,)),
    ]
    vmem = pl.BlockSpec(memory_space=pltpu.VMEM)
    anywhere = pl.BlockSpec(memory_space=pl.ANY)
    loss, grad_hidden, grad_head = pl.pallas_call(
        kernel,
        out_shape=(
            jax.ShapeDtypeStruct((1, 1), F32),
            jax.ShapeDtypeStruct((rows, width), BF16),
            jax.ShapeDtypeStruct((share // PEERS, bottleneck), F32),
        ),
        in_specs=[anywhere] * 6,
        out_specs=(vmem, anywhere, vmem),
        scratch_shapes=scratch,
        compiler_params=pltpu.CompilerParams(
            collective_id=0, has_side_effects=True, vmem_limit_bytes=60 * 1024 * 1024
        ),
        name="ibot",
    )(
        masks,
        hidden_states,
        teacher_feats,
        head_weight,
        prototypes,
        center.reshape(-1, 128),
    )
    def hand(*refs):
        for source, target in zip(refs[:3], refs[3:]):
            target[...] = source[...]

    loss, grad_hidden, grad_head = pl.pallas_call(
        hand,
        out_shape=tuple(
            jax.ShapeDtypeStruct(part.shape, part.dtype) for part in (loss, grad_hidden, grad_head)
        ),
        name="hand",
    )(loss, grad_hidden, grad_head)
    return (loss.reshape(()), grad_hidden, grad_head)


def solution(mesh):
    finer = Mesh(mesh.devices.reshape(DP, NX, NZ), DP_PROTO)
    placed = (
        P(DP_PROTO, None, None),
        P(DP_PROTO, None, None),
        P(DP_PROTO, None),
        P(),
        P(PROTO, None),
        P(PROTO),
    )
    return jax.shard_map(
        per_device,
        mesh=finer,
        in_specs=placed,
        out_specs=(P(), P(DP_PROTO, None), P(DP_PROTO, None)),
        check_vma=False,
    )
```

```python
import math

import jax
import jax.numpy as jnp
from jax import lax
from jax.experimental import pallas as pl
from jax.experimental.pallas import tpu as pltpu
from jax.sharding import Mesh
from jax.sharding import PartitionSpec as P

PROTO = ("proto_0", "proto_1")
DP_PROTO = ("dp", "proto_0", "proto_1")

STUDENT_TEMP = 0.1
TEACHER_TEMP = 0.07
LOSS_SCALE = 524288.0
EPSILON = 1e-06

LOG2E = 1.4426950408889634
LN2 = 0.6931471805599453
S_FACTOR = LOG2E / STUDENT_TEMP
T_FACTOR = LOG2E / TEACHER_TEMP

F32 = jnp.float32
BF16 = jnp.bfloat16
MESH = pl.DeviceIdType.MESH

DP = 16
NX = 2
NZ = 8
PEERS = NX * NZ
TILE = 1536
PART = 256
KTILE = 256


def contract(left, right, dims):
    return lax.dot_general(left, right, (dims, ((), ())), preferred_element_type=F32)


def kernel(
    masks_hbm,
    hidden_hbm,
    teacher_hbm,
    weight_hbm,
    protos_hbm,
    center_hbm,
    loss_out,
    hidden_out,
    head_out,
    masks,
    center,
    hidden_rows,
    hidden,
    feats,
    weight,
    protos,
    protos_t,
    centers,
    rows_all,
    s_even,
    s_odd,
    t_even,
    t_odd,
    unit_ref,
    radius_ref,
    picked_mine,
    picked_all,
    stats,
    stats_all,
    top,
    parts,
    side_in,
    up_in,
    down_in,
    up_other,
    down_other,
    dirs,
    losses,
    losses_p,
    heads,
    heads_all,
    heads_full,
    turned_picks,
    load_sem,
    row_send,
    row_recv,
    pick_send,
    pick_recv,
    stat_send,
    stat_recv,
    side_send,
    side_recv,
    up_send,
    up_recv,
    down_send,
    down_recv,
    upo_send,
    upo_recv,
    downo_send,
    downo_recv,
    dir_send,
    dir_recv,
    pass_send,
    loss_send,
    loss_recv,
    lossp_send,
    lossp_recv,
    head_send,
    head_recv,
    ready,
):
    d = lax.axis_index("dp")
    a = lax.axis_index("proto_0")
    z = lax.axis_index("proto_1")
    b = 1 - a
    p = a * NZ + z
    images, patches, _ = hidden.shape
    picks = masks.shape[1]
    rows = images * picks
    bottleneck = weight.shape[1]
    table = protos.shape[0]
    tiles = table // TILE
    lines = PART // 8
    cuts = TILE // PART
    pending = []

    def send(src, dst, send_sem, recv_sem, device):
        copy = pltpu.make_async_remote_copy(
            src_ref=src,
            dst_ref=dst,
            send_sem=send_sem,
            recv_sem=recv_sem,
            device_id=device,
            device_id_type=MESH,
        )
        copy.start()
        pending.append(copy)

    def arrived(ref, sem):
        pltpu.make_async_remote_copy(
            src_ref=ref,
            dst_ref=ref,
            send_sem=sem,
            recv_sem=sem,
            device_id={"proto_0": b},
            device_id_type=MESH,
        ).wait_recv()

    places = sorted(
        ((x, line) for x in range(NX) for line in range(NZ) if x or line),
        key=lambda place: -(place[0] + min(place[1], NZ - place[1])),
    )

    def proto_peer(k):
        x, line = places[k - 1]
        column, line = (b if x else a), (z + line) % NZ
        return column * NZ + line, {"proto_0": column, "proto_1": line}

    def dp_peer(k):
        peer = (d + k) % DP
        return peer, {"dp": peer}

    barrier = pltpu.get_barrier_semaphore()
    above = {"proto_1": (z + 1) % NZ}
    below = {"proto_1": (z + NZ - 1) % NZ}
    beside = {"proto_0": b}
    partners = [{"dp": d + bit * (1 - 2 * ((d // bit) % 2))} for bit in (1, 2, 4, 8)]
    greeted = [above, below, beside, *partners]
    for device in greeted:
        pl.semaphore_signal(barrier, inc=1, device_id=device, device_id_type=MESH)

    loads = [
        pltpu.make_async_copy(src, dst, load_sem.at[k])
        for k, (src, dst) in enumerate(
            (
                (hidden_hbm, hidden),
                (weight_hbm, weight),
                (teacher_hbm, feats),
                (protos_hbm, protos),
                (masks_hbm, masks),
                (center_hbm, center),
            )
        )
    ]
    for load in (loads[4], *loads[:4], loads[5]):
        load.start()

    loads[4].wait()
    loads[0].wait()
    loads[1].wait()
    loads[2].wait()
    picked_parts = []
    teacher_parts = []
    for image in range(images):
        index = lax.broadcasted_iota(jnp.int32, (patches, picks), 0)
        hot = (index == masks[image : image + 1, :]).astype(F32).astype(BF16)
        picked_parts.append(contract(hot, hidden[image], ((0,), (0,))).astype(BF16))
        teacher_parts.append(contract(hot, feats[image], ((0,), (0,))))
    picked = jnp.concatenate(picked_parts, axis=0)
    chosen = jnp.concatenate(teacher_parts, axis=0)
    raw = contract(picked, weight[...], ((1,), (0,)))
    radius = jnp.sqrt(jnp.sum(raw * raw, axis=1, keepdims=True) + EPSILON)
    unit = raw / radius
    unit_ref[...] = unit
    radius_ref[...] = jnp.broadcast_to(radius, radius_ref.shape)
    length = jnp.sqrt(jnp.sum(chosen * chosen, axis=1, keepdims=True) + EPSILON)
    rows_all[z, a] = unit.astype(BF16)
    rows_all[z, 2 + a] = (chosen / length).astype(BF16)
    share = picked_mine.shape[2]
    for k in range(DP):
        picked_mine[k] = picked[:, k * share : (k + 1) * share]

    pl.semaphore_wait(barrier, len(greeted))

    above_two = {"proto_1": (z + 2) % NZ}
    below_two = {"proto_1": (z + NZ - 2) % NZ}
    row_count = []

    def at(step):
        return (z + step) % NZ

    small = rows // 2

    def slot(other, step, piece):
        kind, side = divmod(piece, 2)
        column = (b if other else a) + 2 * kind
        here = pl.ds(side * small, small)
        return rows_all.at[at(step % NZ), column, here], row_recv.at[at(step % NZ), column, side]

    def row_pass(other, step, piece, device):
        ref, sem = slot(other, step, piece)
        send(ref, ref, row_send.at[len(row_count)], sem, device)
        row_count.append(0)

    def row_wait(other, step, piece):
        ref, sem = slot(other, step, piece)
        arrived(ref, sem)

    every_piece = range(4)
    for piece in every_piece:
        row_pass(0, 0, piece, beside)
        row_pass(0, 0, piece, above)
        row_pass(0, 0, piece, below)

    def tell(turn):
        pl.semaphore_signal(
            ready.at[turn], inc=1, device_id=partners[turn], device_id_type=MESH
        )

    tell(0)
    loads[3].wait()
    loads[5].wait()
    for index in range(table // 256):
        protos_t[index] = protos[index * 256 : (index + 1) * 256, :].T
    for index in range(table // 128):
        column = jnp.broadcast_to(center[index : index + 1, :], (128, 128)).T
        centers[index * 16 : (index + 1) * 16] = column.reshape(16, 8, 128)

    def down(ref):
        return jnp.broadcast_to(ref, (8, 128))

    order = (0, 1, 7, 2, 6, 3, 5, 4)

    def held(step):
        place = order.index(step)
        refs = (s_odd, t_odd) if place % 2 else (s_even, t_even)
        return tuple(ref.at[place // 2] for ref in refs)

    def logits_tile(index, step, state):
        peak_s, peak_t = state
        s_ref, t_ref = held(step)
        first = pl.multiple_of(index * PART, PART)
        tile = protos[pl.ds(first, PART), :]
        both = contract(tile, rows_all[at(step)].reshape(4 * rows, bottleneck), ((1,), (1,)))
        at_line = pl.ds(index * lines, lines)
        s = both[:, : 2 * rows].reshape(lines, 8, 128)
        t = both[:, 2 * rows :].reshape(lines, 8, 128) - centers[at_line]
        s_ref[at_line] = s
        t_ref[at_line] = t
        return jnp.maximum(peak_s, jnp.max(s, axis=0)), jnp.maximum(peak_t, jnp.max(t, axis=0))

    def weights_tile(index, step, peaks, state):
        total_s, total_t, cross = state
        s_ref, t_ref = held(step)
        at_line = pl.ds(index * lines, lines)
        s = s_ref[at_line]
        power_s = jnp.exp2((s - peaks[0]) * S_FACTOR)
        power_t = jnp.exp2((t_ref[at_line] - peaks[1]) * T_FACTOR)
        s_ref[at_line] = power_s
        t_ref[at_line] = power_t
        return (
            total_s + jnp.sum(power_s, axis=0),
            total_t + jnp.sum(power_t, axis=0),
            cross + jnp.sum(power_t * s, axis=0),
        )

    lowest = (jnp.full((8, 128), -jnp.inf, F32),) * 2
    zeros = (jnp.zeros((8, 128), F32),) * 3

    def peaks_of(state):
        return tuple(down(jnp.max(part, axis=0, keepdims=True)) for part in state)

    def finish(step, peaks, state):
        total_s, total_t, cross = (jnp.sum(part, axis=0, keepdims=True) for part in state)
        here = pl.ds(at(step), 1)
        shift_s = peaks[0][:1] * S_FACTOR
        shift_t = peaks[1][:1] * T_FACTOR
        top[0, here, :] = shift_s
        top[1, here, :] = shift_t
        top[2, here, :] = cross / total_t
        stats[0, here, :] = shift_s + jnp.log(total_s) * LOG2E
        stats[1, here, :] = shift_t + jnp.log(total_t) * LOG2E

    def many(index, state, work, *given):
        for k in range(cuts):
            state = work(index * cuts + k, *given, state)
        return state

    def first_pair(line):
        return peaks_of(
            lax.fori_loop(0, tiles, lambda i, state: many(i, state, logits_tile, line), lowest)
        )

    def pair(line, before, peaks):
        def body(index, state):
            new, sums = state
            for k in range(cuts):
                new = logits_tile(index * cuts + k, line, new)
                sums = weights_tile(index * cuts + k, before, peaks, sums)
            return new, sums

        new, sums = lax.fori_loop(0, tiles, body, (lowest, zeros))
        finish(before, peaks, sums)
        return peaks_of(new)

    def last_pair(before, peaks):
        sums = lax.fori_loop(
            0, tiles, lambda i, state: many(i, state, weights_tile, before, peaks), zeros
        )
        finish(before, peaks, sums)

    for piece in every_piece:
        for step, device in ((1, below), (-1, above)):
            row_wait(0, step, piece)
            row_pass(0, step, piece, device)
            row_pass(0, step, piece, beside)
    for piece in every_piece:
        row_wait(1, 0, piece)
    pl.semaphore_wait(ready.at[0], 1)
    tell(1)
    peaks = first_pair(0)
    pl.semaphore_wait(ready.at[1], 1)
    tell(2)
    for piece in every_piece:
        for step, device in ((2, below), (-2, above)):
            row_wait(0, step, piece)
            row_pass(0, step, piece, device)
    for piece in every_piece:
        for step, device in ((1, below), (-1, above)):
            row_wait(1, step, piece)
            row_pass(1, step, piece, device)
    peaks = pair(1, 0, peaks)
    pl.semaphore_wait(ready.at[2], 1)
    for piece in every_piece:
        for step, device in ((3, below), (-3, above)):
            row_wait(0, step, piece)
            if (piece < 2) == (step > 0):
                row_pass(0, step, piece, device)
            row_pass(0, step, piece, beside)
    peaks = pair(7, 1, peaks)
    for piece in every_piece:
        row_wait(1, 2, piece)
    peaks = pair(2, 7, peaks)
    for piece in (0, 2, 1, 3):
        row_wait(0, 4, piece)
        row_pass(0, 4, piece, beside)
    for piece in every_piece:
        row_wait(1, -2, piece)
    peaks = pair(6, 2, peaks)
    for piece in every_piece:
        row_wait(1, 3, piece)
    peaks = pair(3, 6, peaks)
    for piece in every_piece:
        row_wait(1, -3, piece)
    peaks = pair(5, 3, peaks)
    for piece in every_piece:
        row_wait(1, 4, piece)
    peaks = pair(4, 5, peaks)
    last_pair(4, peaks)

    for k in range(1, PEERS):
        peer, device = proto_peer(k)
        send(stats, stats_all.at[p], stat_send.at[k], stat_recv.at[p], device)
    for k in range(1, DP):
        peer, device = dp_peer(k)
        send(picked_mine.at[peer], picked_all.at[d], pick_send.at[k], pick_recv.at[d], device)
    picked_all[d] = picked_mine[d]
    stats_all[p] = stats[...]
    for k in range(1, PEERS):
        peer = (p + k) % PEERS
        arrived(stats_all.at[peer], stat_recv.at[peer])
    every = stats_all[...]
    highest = jnp.max(every, axis=0)
    joined = highest + jnp.log(jnp.sum(jnp.exp2(every - highest), axis=0)) * LOG2E
    total_rows = rows * PEERS * DP
    factor = math.log2(LOSS_SCALE / (total_rows * STUDENT_TEMP))
    losses[d] = joined[0] * (LN2 / PEERS) - top[2] * jnp.exp2(stats[1] - joined[1]) / STUDENT_TEMP
    top[0] = jnp.exp2(top[0] - joined[0] + factor)
    top[1] = jnp.exp2(top[1] - joined[1] + factor)

    def part_of(step, chunk):
        s_ref, t_ref = held(step)
        here = pl.ds(chunk * (KTILE // 8), KTILE // 8)
        up = down(top[0, pl.ds(at(step), 1), :])
        off = down(top[1, pl.ds(at(step), 1), :])
        value = s_ref[here] * up - t_ref[here] * off
        return value.reshape(KTILE, 128).astype(BF16)

    def back_of(far, near):
        product = None
        for chunk in range(table // KTILE):
            right = jnp.concatenate([part_of(far, chunk), part_of(near, chunk)], axis=1)
            left = jnp.concatenate(
                [protos_t[chunk * (KTILE // 256) + k] for k in range(KTILE // 256)], axis=1
            )
            piece = contract(left, right, ((1,), (0,)))
            product = piece if product is None else product + piece
        turned = product.T
        parts[far] = turned[: 2 * rows].reshape(2, rows, bottleneck)
        parts[near] = turned[2 * rows :].reshape(2, rows, bottleneck)

    quarter = rows // 4

    def cut(piece):
        return pl.ds(piece * quarter, quarter)

    def give_side(step):
        for piece in every_piece:
            send(
                parts.at[step, b, cut(piece)],
                side_in.at[step, cut(piece)],
                side_send.at[step, piece],
                side_recv.at[step, piece],
                beside,
            )

    def give_along(column, step, piece, target, sems, device):
        send(
            parts.at[step, column, cut(piece)],
            target.at[cut(piece)],
            sems[0].at[piece],
            sems[1].at[piece],
            device,
        )

    def take(column, step, piece, source, sem):
        arrived(source.at[cut(piece)], sem.at[piece])
        parts[step, column, cut(piece)] += source[cut(piece)]

    def take_side(step, piece):
        take(a, step, piece, side_in.at[step], side_recv.at[step])

    def up(step, piece):
        k = step - 1
        device = above_two if step == 2 else above
        give_along(a, step, piece, up_in.at[k], (up_send.at[k], up_recv.at[k]), device)

    def low(step, piece):
        k = (-step) % NZ - 1
        device = below_two if step == 6 else below
        give_along(a, step, piece, down_in.at[k], (down_send.at[k], down_recv.at[k]), device)

    back_of(4, 3)
    give_side(4)
    give_side(3)
    back_of(5, 2)
    give_side(5)
    for piece in every_piece:
        give_along(b, 2, piece, up_other, (upo_send, upo_recv), above)
    back_of(6, 1)
    for piece in every_piece:
        give_along(b, 6, piece, down_other, (downo_send, downo_recv), below)
    for piece in (0, 1):
        take_side(4, piece)
        up(4, piece)
    for piece in (2, 3):
        take_side(4, piece)
        low(4, piece)
    back_of(7, 0)
    give_side(0)
    for piece in (2, 3):
        take_side(3, piece)
        up(3, piece)
        take_side(5, piece - 2)
        low(5, piece - 2)
    for piece in every_piece:
        take(b, 1, piece, up_other, upo_recv)
        take(b, 7, piece, down_other, downo_recv)
    give_side(1)
    give_side(7)
    for piece in (0, 1):
        take_side(3, piece)
        take(a, 3, piece, up_in.at[3], up_recv.at[3])
        up(3, piece)
        take_side(5, piece + 2)
        take(a, 5, piece + 2, down_in.at[3], down_recv.at[3])
        low(5, piece + 2)
    for piece in every_piece:
        turned_piece = (piece + 2) % 4
        take(a, 2, turned_piece, up_in.at[2], up_recv.at[2])
        up(2, turned_piece)
        take(a, 6, piece, down_in.at[2], down_recv.at[2])
        low(6, piece)
    for piece in every_piece:
        take_side(1, piece)
        up(1, piece)
        take_side(7, piece)
        low(7, piece)
    for piece in every_piece:
        take_side(0, piece)
        take(a, 0, piece, up_in.at[0], up_recv.at[0])
        take(a, 0, piece, down_in.at[0], down_recv.at[0])
        take(a, 0, piece, up_in.at[1], up_recv.at[1])
        take(a, 0, piece, down_in.at[1], down_recv.at[1])
    back = parts[0, a]

    unit = unit_ref[...]
    inner = jnp.sum(unit * back, axis=1, keepdims=True)
    direction = ((back - unit * inner) / radius_ref[:, :1]).astype(BF16)
    dirs[d] = direction

    pair_core = d + 1 - 2 * (d % 2)
    def chip_peer(y_step, x_step):
        return (d + 4 * y_step) % DP + 2 * x_step * (1 - 2 * ((d // 2) % 2))

    chips = ((2, 1), (1, 1), (3, 1), (0, 1), (2, 0), (1, 0), (3, 0))
    for k, steps in enumerate(chips):
        send(
            dirs.at[d], dirs.at[d], dir_send.at[k + 1], dir_recv.at[d], {"dp": chip_peer(*steps)}
        )
    send(dirs.at[d], dirs.at[d], dir_send.at[0], dir_recv.at[d], {"dp": pair_core})
    for k in range(1, DP):
        peer, device = dp_peer(k)
        send(losses.at[d], losses.at[d], loss_send.at[k], loss_recv.at[d], device)

    hidden_rows[...] = contract(direction, weight[...], ((1,), (1,))).astype(BF16)
    store = pltpu.make_async_copy(hidden_rows, hidden_out, load_sem.at[0])
    store.start()

    for k, steps in enumerate(chips[5:] + chips[4:5] + chips[:4]):
        peer = chip_peer(*steps)
        arrived(dirs.at[peer], dir_recv.at[peer])
        send(
            dirs.at[peer],
            dirs.at[peer],
            pass_send.at[k + 1],
            dir_recv.at[peer],
            {"dp": pair_core},
        )
    for k in range(1, DP):
        peer = (d + k) % DP
        arrived(losses.at[peer], loss_recv.at[peer])
        arrived(picked_all.at[peer], pick_recv.at[peer])
    losses_p[p] = jnp.sum(losses[...], axis=0)
    for k in range(1, PEERS):
        peer, device = proto_peer(k)
        send(losses_p.at[p], losses_p.at[p], lossp_send.at[k], lossp_recv.at[p], device)
    turned_picks[...] = picked_all[...].reshape(DP * rows, share).T
    for k in range(DP // 2):
        peer = (pair_core + 2 * k) % DP
        arrived(dirs.at[peer], dir_recv.at[peer])

    share_rows = heads.shape[1]
    product = contract(
        turned_picks[...], dirs[...].reshape(DP * rows, bottleneck), ((1,), (0,))
    )
    product = product.reshape(PEERS, share_rows, bottleneck)
    heads_full[...] = product
    heads[...] = product.astype(BF16)
    for k in range(1, PEERS):
        peer, device = proto_peer(k)
        send(heads.at[peer], heads_all.at[p], head_send.at[k], head_recv.at[p], device)
    result = heads_full[p]
    loss = losses_p[p]
    for k in range(1, PEERS):
        peer = (p + k) % PEERS
        arrived(losses_p.at[peer], lossp_recv.at[peer])
        loss = loss + losses_p[peer]
        arrived(heads_all.at[peer], head_recv.at[peer])
        result = result + heads_all[peer].astype(F32)
    head_out[...] = result
    loss = jnp.sum(jnp.sum(loss, axis=0, keepdims=True), axis=1, keepdims=True)
    loss_out[...] = loss / total_rows

    store.wait()
    for copy in pending:
        copy.wait_send()


def per_device(hidden_states, teacher_feats, masks, head_weight, prototypes, center):
    images, patches, width = hidden_states.shape
    bottleneck = head_weight.shape[1]
    table = prototypes.shape[0]
    rows = masks.shape[0] * masks.shape[1]
    share = width // DP
    dma = pltpu.SemaphoreType.DMA
    scratch = [
        pltpu.VMEM(masks.shape, jnp.int32),
        pltpu.VMEM((table // 128, 128), F32),
        pltpu.VMEM((rows, width), BF16),
        pltpu.VMEM(hidden_states.shape, BF16),
        pltpu.VMEM(teacher_feats.shape, BF16),
        pltpu.VMEM(head_weight.shape, BF16),
        pltpu.VMEM(prototypes.shape, BF16),
        pltpu.VMEM((table // 256, bottleneck, 256), BF16),
        pltpu.VMEM((table // 8, 8, 128), F32),
        pltpu.VMEM((NZ, 4, rows, bottleneck), BF16),
        pltpu.VMEM((NZ // 2, table // 8, 8, 128), F32),
        pltpu.VMEM((NZ // 2, table // 8, 8, 128), F32),
        pltpu.VMEM((NZ // 2, table // 8, 8, 128), F32),
        pltpu.VMEM((NZ // 2, table // 8, 8, 128), F32),
        pltpu.VMEM((rows, bottleneck), F32),
        pltpu.VMEM((rows, 128), F32),
        pltpu.VMEM((DP, rows, share), BF16),
        pltpu.VMEM((DP, rows, share), BF16),
        pltpu.VMEM((2, 8, 128), F32),
        pltpu.VMEM((PEERS, 2, 8, 128), F32),
        pltpu.VMEM((3, 8, 128), F32),
        pltpu.VMEM((NZ, 2, rows, bottleneck), F32),
        pltpu.VMEM((NZ, rows, bottleneck), F32),
        pltpu.VMEM((4, rows, bottleneck), F32),
        pltpu.VMEM((4, rows, bottleneck), F32),
        pltpu.VMEM((rows, bottleneck), F32),
        pltpu.VMEM((rows, bottleneck), F32),
        pltpu.VMEM((DP, rows, bottleneck), BF16),
        pltpu.VMEM((DP, 8, 128), F32),
        pltpu.VMEM((PEERS, 8, 128), F32),
        pltpu.VMEM((PEERS, share // PEERS, bottleneck), BF16),
        pltpu.VMEM((PEERS, share // PEERS, bottleneck), BF16),
        pltpu.VMEM((PEERS, share // PEERS, bottleneck), F32),
        pltpu.VMEM((share, DP * rows), BF16),
        dma((6,)),
        dma((64,)),
        dma((NZ, 4, 2)),
        dma((DP,)),
        dma((DP,)),
        dma((PEERS,)),
        dma((PEERS,)),
        dma((NZ, 4)),
        dma((NZ, 4)),
        dma((4, 4)),
        dma((4, 4)),
        dma((4, 4)),
        dma((4, 4)),
        dma((4,)),
        dma((4,)),
        dma((4,)),
        dma((4,)),
        dma((DP // 2,)),
        dma((DP,)),
        dma((DP // 2,)),
        dma((DP,)),
        dma((DP,)),
        dma((PEERS,)),
        dma((PEERS,)),
        dma((PEERS,)),
        dma((PEERS,)),
        pltpu.SemaphoreType.REGULAR((3,)),
    ]
    vmem = pl.BlockSpec(memory_space=pltpu.VMEM)
    anywhere = pl.BlockSpec(memory_space=pl.ANY)
    loss, grad_hidden, grad_head = pl.pallas_call(
        kernel,
        out_shape=(
            jax.ShapeDtypeStruct((1, 1), F32),
            jax.ShapeDtypeStruct((rows, width), BF16),
            jax.ShapeDtypeStruct((share // PEERS, bottleneck), F32),
        ),
        in_specs=[anywhere] * 6,
        out_specs=(vmem, anywhere, vmem),
        scratch_shapes=scratch,
        compiler_params=pltpu.CompilerParams(
            collective_id=0, has_side_effects=True, vmem_limit_bytes=60 * 1024 * 1024
        ),
        name="ibot",
    )(
        masks,
        hidden_states,
        teacher_feats,
        head_weight,
        prototypes,
        center.reshape(-1, 128),
    )
    def hand(*refs):
        for source, target in zip(refs[:3], refs[3:]):
            target[...] = source[...]

    loss, grad_hidden, grad_head = pl.pallas_call(
        hand,
        out_shape=tuple(
            jax.ShapeDtypeStruct(part.shape, part.dtype) for part in (loss, grad_hidden, grad_head)
        ),
        name="hand",
    )(loss, grad_hidden, grad_head)
    return (loss.reshape(()), grad_hidden, grad_head)


def solution(mesh):
    finer = Mesh(mesh.devices.reshape(DP, NX, NZ), DP_PROTO)
    placed = (
        P(DP_PROTO, None, None),
        P(DP_PROTO, None, None),
        P(DP_PROTO, None),
        P(),
        P(PROTO, None),
        P(PROTO),
    )
    return jax.shard_map(
        per_device,
        mesh=finer,
        in_specs=placed,
        out_specs=(P(), P(DP_PROTO, None), P(DP_PROTO, None)),
        check_vma=False,
    )
```

```python
import math

import jax
import jax.numpy as jnp
from jax import lax
from jax.experimental import pallas as pl
from jax.experimental.pallas import tpu as pltpu
from jax.sharding import Mesh
from jax.sharding import PartitionSpec as P

PROTO = ("proto_0", "proto_1")
DP_PROTO = ("dp", "proto_0", "proto_1")

STUDENT_TEMP = 0.1
TEACHER_TEMP = 0.07
LOSS_SCALE = 524288.0
EPSILON = 1e-06

LOG2E = 1.4426950408889634
LN2 = 0.6931471805599453
S_FACTOR = LOG2E / STUDENT_TEMP
T_FACTOR = LOG2E / TEACHER_TEMP

F32 = jnp.float32
BF16 = jnp.bfloat16
MESH = pl.DeviceIdType.MESH

DP = 16
NX = 2
NZ = 8
PEERS = NX * NZ
TILE = 1536
PART = 256
KTILE = 256


def contract(left, right, dims):
    return lax.dot_general(left, right, (dims, ((), ())), preferred_element_type=F32)


def kernel(
    masks_hbm,
    hidden_hbm,
    teacher_hbm,
    weight_hbm,
    protos_hbm,
    center_hbm,
    loss_out,
    hidden_out,
    head_out,
    masks,
    center,
    hidden_rows,
    hidden,
    feats,
    weight,
    protos,
    protos_t,
    centers,
    rows_all,
    s_even,
    s_odd,
    t_even,
    t_odd,
    unit_ref,
    radius_ref,
    picked_mine,
    picked_all,
    stats,
    stats_all,
    top,
    parts,
    side_in,
    up_in,
    down_in,
    up_other,
    down_other,
    dirs,
    losses,
    losses_p,
    heads,
    heads_all,
    heads_full,
    turned_picks,
    load_sem,
    row_send,
    row_recv,
    pick_send,
    pick_recv,
    stat_send,
    stat_recv,
    side_send,
    side_recv,
    up_send,
    up_recv,
    down_send,
    down_recv,
    upo_send,
    upo_recv,
    downo_send,
    downo_recv,
    dir_send,
    dir_recv,
    pass_send,
    loss_send,
    loss_recv,
    lossp_send,
    lossp_recv,
    head_send,
    head_recv,
    ready,
):
    d = lax.axis_index("dp")
    a = lax.axis_index("proto_0")
    z = lax.axis_index("proto_1")
    b = 1 - a
    p = a * NZ + z
    images, patches, _ = hidden.shape
    picks = masks.shape[1]
    rows = images * picks
    bottleneck = weight.shape[1]
    table = protos.shape[0]
    tiles = table // TILE
    lines = PART // 8
    cuts = TILE // PART
    pending = []

    def send(src, dst, send_sem, recv_sem, device):
        copy = pltpu.make_async_remote_copy(
            src_ref=src,
            dst_ref=dst,
            send_sem=send_sem,
            recv_sem=recv_sem,
            device_id=device,
            device_id_type=MESH,
        )
        copy.start()
        pending.append(copy)

    def arrived(ref, sem):
        pltpu.make_async_remote_copy(
            src_ref=ref,
            dst_ref=ref,
            send_sem=sem,
            recv_sem=sem,
            device_id={"proto_0": b},
            device_id_type=MESH,
        ).wait_recv()

    places = sorted(
        ((x, line) for x in range(NX) for line in range(NZ) if x or line),
        key=lambda place: -(place[0] + min(place[1], NZ - place[1])),
    )

    def proto_peer(k):
        x, line = places[k - 1]
        column, line = (b if x else a), (z + line) % NZ
        return column * NZ + line, {"proto_0": column, "proto_1": line}

    def dp_peer(k):
        peer = (d + k) % DP
        return peer, {"dp": peer}

    barrier = pltpu.get_barrier_semaphore()
    above = {"proto_1": (z + 1) % NZ}
    below = {"proto_1": (z + NZ - 1) % NZ}
    beside = {"proto_0": b}
    partners = [{"dp": d + bit * (1 - 2 * ((d // bit) % 2))} for bit in (1, 2, 4, 8)]
    greeted = [above, below, beside, *partners]
    for device in greeted:
        pl.semaphore_signal(barrier, inc=1, device_id=device, device_id_type=MESH)

    loads = [
        pltpu.make_async_copy(src, dst, load_sem.at[k])
        for k, (src, dst) in enumerate(
            (
                (hidden_hbm, hidden),
                (weight_hbm, weight),
                (teacher_hbm, feats),
                (protos_hbm, protos),
                (masks_hbm, masks),
                (center_hbm, center),
            )
        )
    ]
    for load in (loads[4], loads[2], *loads[:2], loads[3], loads[5]):
        load.start()

    loads[4].wait()
    loads[0].wait()
    loads[1].wait()
    loads[2].wait()
    picked_parts = []
    teacher_parts = []
    for image in range(images):
        index = lax.broadcasted_iota(jnp.int32, (patches, picks), 0)
        hot = (index == masks[image : image + 1, :]).astype(F32).astype(BF16)
        picked_parts.append(contract(hot, hidden[image], ((0,), (0,))).astype(BF16))
        teacher_parts.append(contract(hot, feats[image], ((0,), (0,))))
    picked = jnp.concatenate(picked_parts, axis=0)
    chosen = jnp.concatenate(teacher_parts, axis=0)
    raw = contract(picked, weight[...], ((1,), (0,)))
    radius = jnp.sqrt(jnp.sum(raw * raw, axis=1, keepdims=True) + EPSILON)
    unit = raw / radius
    unit_ref[...] = unit
    radius_ref[...] = jnp.broadcast_to(radius, radius_ref.shape)
    length = jnp.sqrt(jnp.sum(chosen * chosen, axis=1, keepdims=True) + EPSILON)
    rows_all[z, a] = unit.astype(BF16)
    rows_all[z, 2 + a] = (chosen / length).astype(BF16)
    share = picked_mine.shape[2]
    for k in range(DP):
        picked_mine[k] = picked[:, k * share : (k + 1) * share]

    pl.semaphore_wait(barrier, len(greeted))

    above_two = {"proto_1": (z + 2) % NZ}
    below_two = {"proto_1": (z + NZ - 2) % NZ}
    row_count = []

    def at(step):
        return (z + step) % NZ

    small = rows // 2

    def slot(other, step, piece):
        kind, side = divmod(piece, 2)
        column = (b if other else a) + 2 * kind
        here = pl.ds(side * small, small)
        return rows_all.at[at(step % NZ), column, here], row_recv.at[at(step % NZ), column, side]

    def row_pass(other, step, piece, device):
        ref, sem = slot(other, step, piece)
        send(ref, ref, row_send.at[len(row_count)], sem, device)
        row_count.append(0)

    def row_wait(other, step, piece):
        ref, sem = slot(other, step, piece)
        arrived(ref, sem)

    every_piece = range(4)
    arrival = (2, 3, 0, 1)
    for piece in arrival:
        row_pass(0, 0, piece, beside)
        row_pass(0, 0, piece, above)
        row_pass(0, 0, piece, below)

    def tell(turn):
        pl.semaphore_signal(
            ready.at[turn], inc=1, device_id=partners[turn], device_id_type=MESH
        )

    tell(0)
    loads[3].wait()
    loads[5].wait()
    for index in range(table // 256):
        protos_t[index] = protos[index * 256 : (index + 1) * 256, :].T
    for index in range(table // 128):
        column = jnp.broadcast_to(center[index : index + 1, :], (128, 128)).T
        centers[index * 16 : (index + 1) * 16] = column.reshape(16, 8, 128)

    def down(ref):
        return jnp.broadcast_to(ref, (8, 128))

    order = (0, 1, 7, 2, 6, 3, 5, 4)

    def held(step):
        place = order.index(step)
        refs = (s_odd, t_odd) if place % 2 else (s_even, t_even)
        return tuple(ref.at[place // 2] for ref in refs)

    def logits_tile(index, step, state):
        peak_s, peak_t = state
        s_ref, t_ref = held(step)
        first = pl.multiple_of(index * PART, PART)
        tile = protos[pl.ds(first, PART), :]
        both = contract(tile, rows_all[at(step)].reshape(4 * rows, bottleneck), ((1,), (1,)))
        at_line = pl.ds(index * lines, lines)
        s = both[:, : 2 * rows].reshape(lines, 8, 128)
        t = both[:, 2 * rows :].reshape(lines, 8, 128) - centers[at_line]
        s_ref[at_line] = s
        t_ref[at_line] = t
        return jnp.maximum(peak_s, jnp.max(s, axis=0)), jnp.maximum(peak_t, jnp.max(t, axis=0))

    def weights_tile(index, step, peaks, state):
        total_s, total_t, cross = state
        s_ref, t_ref = held(step)
        at_line = pl.ds(index * lines, lines)
        s = s_ref[at_line]
        power_s = jnp.exp2((s - peaks[0]) * S_FACTOR)
        power_t = jnp.exp2((t_ref[at_line] - peaks[1]) * T_FACTOR)
        s_ref[at_line] = power_s
        t_ref[at_line] = power_t
        return (
            total_s + jnp.sum(power_s, axis=0),
            total_t + jnp.sum(power_t, axis=0),
            cross + jnp.sum(power_t * s, axis=0),
        )

    lowest = (jnp.full((8, 128), -jnp.inf, F32),) * 2
    zeros = (jnp.zeros((8, 128), F32),) * 3

    def peaks_of(state):
        return tuple(down(jnp.max(part, axis=0, keepdims=True)) for part in state)

    def finish(step, peaks, state):
        total_s, total_t, cross = (jnp.sum(part, axis=0, keepdims=True) for part in state)
        here = pl.ds(at(step), 1)
        shift_s = peaks[0][:1] * S_FACTOR
        shift_t = peaks[1][:1] * T_FACTOR
        top[0, here, :] = shift_s
        top[1, here, :] = shift_t
        top[2, here, :] = cross / total_t
        stats[0, here, :] = shift_s + jnp.log(total_s) * LOG2E
        stats[1, here, :] = shift_t + jnp.log(total_t) * LOG2E

    def many(index, state, work, *given):
        for k in range(cuts):
            state = work(index * cuts + k, *given, state)
        return state

    def first_pair(line):
        return peaks_of(
            lax.fori_loop(0, tiles, lambda i, state: many(i, state, logits_tile, line), lowest)
        )

    def pair(line, before, peaks):
        def body(index, state):
            new, sums = state
            for k in range(cuts):
                new = logits_tile(index * cuts + k, line, new)
                sums = weights_tile(index * cuts + k, before, peaks, sums)
            return new, sums

        new, sums = lax.fori_loop(0, tiles, body, (lowest, zeros))
        finish(before, peaks, sums)
        return peaks_of(new)

    def last_pair(before, peaks):
        sums = lax.fori_loop(
            0, tiles, lambda i, state: many(i, state, weights_tile, before, peaks), zeros
        )
        finish(before, peaks, sums)

    for piece in arrival:
        for step, device in ((1, below), (-1, above)):
            row_wait(0, step, piece)
            row_pass(0, step, piece, device)
            row_pass(0, step, piece, beside)
    for piece in arrival:
        row_wait(1, 0, piece)
    pl.semaphore_wait(ready.at[0], 1)
    tell(1)
    peaks = first_pair(0)
    pl.semaphore_wait(ready.at[1], 1)
    tell(2)
    for piece in arrival:
        for step, device in ((2, below), (-2, above)):
            row_wait(0, step, piece)
            row_pass(0, step, piece, device)
    for piece in arrival:
        for step, device in ((1, below), (-1, above)):
            row_wait(1, step, piece)
            row_pass(1, step, piece, device)
    peaks = pair(1, 0, peaks)
    pl.semaphore_wait(ready.at[2], 1)
    for piece in arrival:
        for step, device in ((3, below), (-3, above)):
            row_wait(0, step, piece)
            if (piece < 2) == (step > 0):
                row_pass(0, step, piece, device)
            row_pass(0, step, piece, beside)
    peaks = pair(7, 1, peaks)
    for piece in arrival:
        row_wait(1, 2, piece)
    peaks = pair(2, 7, peaks)
    for piece in (0, 2, 1, 3):
        row_wait(0, 4, piece)
        row_pass(0, 4, piece, beside)
    for piece in arrival:
        row_wait(1, -2, piece)
    peaks = pair(6, 2, peaks)
    for piece in arrival:
        row_wait(1, 3, piece)
    peaks = pair(3, 6, peaks)
    for piece in arrival:
        row_wait(1, -3, piece)
    peaks = pair(5, 3, peaks)
    for piece in arrival:
        row_wait(1, 4, piece)
    peaks = pair(4, 5, peaks)
    last_pair(4, peaks)

    for k in range(1, PEERS):
        peer, device = proto_peer(k)
        send(stats, stats_all.at[p], stat_send.at[k], stat_recv.at[p], device)
    for k in range(1, DP):
        peer, device = dp_peer(k)
        send(picked_mine.at[peer], picked_all.at[d], pick_send.at[k], pick_recv.at[d], device)
    picked_all[d] = picked_mine[d]
    stats_all[p] = stats[...]
    for k in range(1, PEERS):
        peer = (p + k) % PEERS
        arrived(stats_all.at[peer], stat_recv.at[peer])
    every = stats_all[...]
    highest = jnp.max(every, axis=0)
    joined = highest + jnp.log(jnp.sum(jnp.exp2(every - highest), axis=0)) * LOG2E
    total_rows = rows * PEERS * DP
    factor = math.log2(LOSS_SCALE / (total_rows * STUDENT_TEMP))
    losses[d] = joined[0] * (LN2 / PEERS) - top[2] * jnp.exp2(stats[1] - joined[1]) / STUDENT_TEMP
    top[0] = jnp.exp2(top[0] - joined[0] + factor)
    top[1] = jnp.exp2(top[1] - joined[1] + factor)

    def part_of(step, chunk):
        s_ref, t_ref = held(step)
        here = pl.ds(chunk * (KTILE // 8), KTILE // 8)
        up = down(top[0, pl.ds(at(step), 1), :])
        off = down(top[1, pl.ds(at(step), 1), :])
        value = s_ref[here] * up - t_ref[here] * off
        return value.reshape(KTILE, 128).astype(BF16)

    def back_of(far, near):
        product = None
        for chunk in range(table // KTILE):
            right = jnp.concatenate([part_of(far, chunk), part_of(near, chunk)], axis=1)
            left = jnp.concatenate(
                [protos_t[chunk * (KTILE // 256) + k] for k in range(KTILE // 256)], axis=1
            )
            piece = contract(left, right, ((1,), (0,)))
            product = piece if product is None else product + piece
        turned = product.T
        parts[far] = turned[: 2 * rows].reshape(2, rows, bottleneck)
        parts[near] = turned[2 * rows :].reshape(2, rows, bottleneck)

    quarter = rows // 4

    def cut(piece):
        return pl.ds(piece * quarter, quarter)

    def give_side(step):
        for piece in every_piece:
            send(
                parts.at[step, b, cut(piece)],
                side_in.at[step, cut(piece)],
                side_send.at[step, piece],
                side_recv.at[step, piece],
                beside,
            )

    def give_along(column, step, piece, target, sems, device):
        send(
            parts.at[step, column, cut(piece)],
            target.at[cut(piece)],
            sems[0].at[piece],
            sems[1].at[piece],
            device,
        )

    def take(column, step, piece, source, sem):
        arrived(source.at[cut(piece)], sem.at[piece])
        parts[step, column, cut(piece)] += source[cut(piece)]

    def take_side(step, piece):
        take(a, step, piece, side_in.at[step], side_recv.at[step])

    def up(step, piece):
        k = step - 1
        device = above_two if step == 2 else above
        give_along(a, step, piece, up_in.at[k], (up_send.at[k], up_recv.at[k]), device)

    def low(step, piece):
        k = (-step) % NZ - 1
        device = below_two if step == 6 else below
        give_along(a, step, piece, down_in.at[k], (down_send.at[k], down_recv.at[k]), device)

    back_of(4, 3)
    give_side(4)
    give_side(3)
    back_of(5, 2)
    give_side(5)
    for piece in every_piece:
        give_along(b, 2, piece, up_other, (upo_send, upo_recv), above)
    back_of(6, 1)
    for piece in every_piece:
        give_along(b, 6, piece, down_other, (downo_send, downo_recv), below)
    for piece in (0, 1):
        take_side(4, piece)
        up(4, piece)
    for piece in (2, 3):
        take_side(4, piece)
        low(4, piece)
    back_of(7, 0)
    give_side(0)
    for piece in (2, 3):
        take_side(3, piece)
        up(3, piece)
        take_side(5, piece - 2)
        low(5, piece - 2)
    for piece in every_piece:
        take(b, 1, piece, up_other, upo_recv)
        take(b, 7, piece, down_other, downo_recv)
    give_side(1)
    give_side(7)
    for piece in (0, 1):
        take_side(3, piece)
        take(a, 3, piece, up_in.at[3], up_recv.at[3])
        up(3, piece)
        take_side(5, piece + 2)
        take(a, 5, piece + 2, down_in.at[3], down_recv.at[3])
        low(5, piece + 2)
    for piece in every_piece:
        turned_piece = (piece + 2) % 4
        take(a, 2, turned_piece, up_in.at[2], up_recv.at[2])
        up(2, turned_piece)
        take(a, 6, piece, down_in.at[2], down_recv.at[2])
        low(6, piece)
    for piece in every_piece:
        take_side(1, piece)
        up(1, piece)
        take_side(7, piece)
        low(7, piece)
    for piece in every_piece:
        take_side(0, piece)
        take(a, 0, piece, up_in.at[0], up_recv.at[0])
        take(a, 0, piece, down_in.at[0], down_recv.at[0])
        take(a, 0, piece, up_in.at[1], up_recv.at[1])
        take(a, 0, piece, down_in.at[1], down_recv.at[1])
    back = parts[0, a]

    unit = unit_ref[...]
    inner = jnp.sum(unit * back, axis=1, keepdims=True)
    direction = ((back - unit * inner) / radius_ref[:, :1]).astype(BF16)
    dirs[d] = direction

    pair_core = d + 1 - 2 * (d % 2)
    def chip_peer(y_step, x_step):
        return (d + 4 * y_step) % DP + 2 * x_step * (1 - 2 * ((d // 2) % 2))

    chips = ((2, 1), (1, 1), (3, 1), (0, 1), (2, 0), (1, 0), (3, 0))
    for k, steps in enumerate(chips):
        send(
            dirs.at[d], dirs.at[d], dir_send.at[k + 1], dir_recv.at[d], {"dp": chip_peer(*steps)}
        )
    send(dirs.at[d], dirs.at[d], dir_send.at[0], dir_recv.at[d], {"dp": pair_core})
    for k in range(1, DP):
        peer, device = dp_peer(k)
        send(losses.at[d], losses.at[d], loss_send.at[k], loss_recv.at[d], device)

    hidden_rows[...] = contract(direction, weight[...], ((1,), (1,))).astype(BF16)
    store = pltpu.make_async_copy(hidden_rows, hidden_out, load_sem.at[0])
    store.start()

    for k, steps in enumerate(chips[5:] + chips[4:5] + chips[:4]):
        peer = chip_peer(*steps)
        arrived(dirs.at[peer], dir_recv.at[peer])
        send(
            dirs.at[peer],
            dirs.at[peer],
            pass_send.at[k + 1],
            dir_recv.at[peer],
            {"dp": pair_core},
        )
    for k in range(1, DP):
        peer = (d + k) % DP
        arrived(losses.at[peer], loss_recv.at[peer])
        arrived(picked_all.at[peer], pick_recv.at[peer])
    losses_p[p] = jnp.sum(losses[...], axis=0)
    for k in range(1, PEERS):
        peer, device = proto_peer(k)
        send(losses_p.at[p], losses_p.at[p], lossp_send.at[k], lossp_recv.at[p], device)
    turned_picks[...] = picked_all[...].reshape(DP * rows, share).T
    for k in range(DP // 2):
        peer = (pair_core + 2 * k) % DP
        arrived(dirs.at[peer], dir_recv.at[peer])

    share_rows = heads.shape[1]
    product = contract(
        turned_picks[...], dirs[...].reshape(DP * rows, bottleneck), ((1,), (0,))
    )
    product = product.reshape(PEERS, share_rows, bottleneck)
    heads_full[...] = product
    heads[...] = product.astype(BF16)
    for k in range(1, PEERS):
        peer, device = proto_peer(k)
        send(heads.at[peer], heads_all.at[p], head_send.at[k], head_recv.at[p], device)
    result = heads_full[p]
    loss = losses_p[p]
    for k in range(1, PEERS):
        peer = (p + k) % PEERS
        arrived(losses_p.at[peer], lossp_recv.at[peer])
        loss = loss + losses_p[peer]
        arrived(heads_all.at[peer], head_recv.at[peer])
        result = result + heads_all[peer].astype(F32)
    head_out[...] = result
    loss = jnp.sum(jnp.sum(loss, axis=0, keepdims=True), axis=1, keepdims=True)
    loss_out[...] = loss / total_rows

    store.wait()
    for copy in pending:
        copy.wait_send()


def per_device(hidden_states, teacher_feats, masks, head_weight, prototypes, center):
    images, patches, width = hidden_states.shape
    bottleneck = head_weight.shape[1]
    table = prototypes.shape[0]
    rows = masks.shape[0] * masks.shape[1]
    share = width // DP
    dma = pltpu.SemaphoreType.DMA
    scratch = [
        pltpu.VMEM(masks.shape, jnp.int32),
        pltpu.VMEM((table // 128, 128), F32),
        pltpu.VMEM((rows, width), BF16),
        pltpu.VMEM(hidden_states.shape, BF16),
        pltpu.VMEM(teacher_feats.shape, BF16),
        pltpu.VMEM(head_weight.shape, BF16),
        pltpu.VMEM(prototypes.shape, BF16),
        pltpu.VMEM((table // 256, bottleneck, 256), BF16),
        pltpu.VMEM((table // 8, 8, 128), F32),
        pltpu.VMEM((NZ, 4, rows, bottleneck), BF16),
        pltpu.VMEM((NZ // 2, table // 8, 8, 128), F32),
        pltpu.VMEM((NZ // 2, table // 8, 8, 128), F32),
        pltpu.VMEM((NZ // 2, table // 8, 8, 128), F32),
        pltpu.VMEM((NZ // 2, table // 8, 8, 128), F32),
        pltpu.VMEM((rows, bottleneck), F32),
        pltpu.VMEM((rows, 128), F32),
        pltpu.VMEM((DP, rows, share), BF16),
        pltpu.VMEM((DP, rows, share), BF16),
        pltpu.VMEM((2, 8, 128), F32),
        pltpu.VMEM((PEERS, 2, 8, 128), F32),
        pltpu.VMEM((3, 8, 128), F32),
        pltpu.VMEM((NZ, 2, rows, bottleneck), F32),
        pltpu.VMEM((NZ, rows, bottleneck), F32),
        pltpu.VMEM((4, rows, bottleneck), F32),
        pltpu.VMEM((4, rows, bottleneck), F32),
        pltpu.VMEM((rows, bottleneck), F32),
        pltpu.VMEM((rows, bottleneck), F32),
        pltpu.VMEM((DP, rows, bottleneck), BF16),
        pltpu.VMEM((DP, 8, 128), F32),
        pltpu.VMEM((PEERS, 8, 128), F32),
        pltpu.VMEM((PEERS, share // PEERS, bottleneck), BF16),
        pltpu.VMEM((PEERS, share // PEERS, bottleneck), BF16),
        pltpu.VMEM((PEERS, share // PEERS, bottleneck), F32),
        pltpu.VMEM((share, DP * rows), BF16),
        dma((6,)),
        dma((64,)),
        dma((NZ, 4, 2)),
        dma((DP,)),
        dma((DP,)),
        dma((PEERS,)),
        dma((PEERS,)),
        dma((NZ, 4)),
        dma((NZ, 4)),
        dma((4, 4)),
        dma((4, 4)),
        dma((4, 4)),
        dma((4, 4)),
        dma((4,)),
        dma((4,)),
        dma((4,)),
        dma((4,)),
        dma((DP // 2,)),
        dma((DP,)),
        dma((DP // 2,)),
        dma((DP,)),
        dma((DP,)),
        dma((PEERS,)),
        dma((PEERS,)),
        dma((PEERS,)),
        dma((PEERS,)),
        pltpu.SemaphoreType.REGULAR((3,)),
    ]
    vmem = pl.BlockSpec(memory_space=pltpu.VMEM)
    anywhere = pl.BlockSpec(memory_space=pl.ANY)
    loss, grad_hidden, grad_head = pl.pallas_call(
        kernel,
        out_shape=(
            jax.ShapeDtypeStruct((1, 1), F32),
            jax.ShapeDtypeStruct((rows, width), BF16),
            jax.ShapeDtypeStruct((share // PEERS, bottleneck), F32),
        ),
        in_specs=[anywhere] * 6,
        out_specs=(vmem, anywhere, vmem),
        scratch_shapes=scratch,
        compiler_params=pltpu.CompilerParams(
            collective_id=0, has_side_effects=True, vmem_limit_bytes=60 * 1024 * 1024
        ),
        name="ibot",
    )(
        masks,
        hidden_states,
        teacher_feats,
        head_weight,
        prototypes,
        center.reshape(-1, 128),
    )
    def hand(*refs):
        for source, target in zip(refs[:3], refs[3:]):
            target[...] = source[...]

    loss, grad_hidden, grad_head = pl.pallas_call(
        hand,
        out_shape=tuple(
            jax.ShapeDtypeStruct(part.shape, part.dtype) for part in (loss, grad_hidden, grad_head)
        ),
        name="hand",
    )(loss, grad_hidden, grad_head)
    return (loss.reshape(()), grad_hidden, grad_head)


def solution(mesh):
    finer = Mesh(mesh.devices.reshape(DP, NX, NZ), DP_PROTO)
    placed = (
        P(DP_PROTO, None, None),
        P(DP_PROTO, None, None),
        P(DP_PROTO, None),
        P(),
        P(PROTO, None),
        P(PROTO),
    )
    return jax.shard_map(
        per_device,
        mesh=finer,
        in_specs=placed,
        out_specs=(P(), P(DP_PROTO, None), P(DP_PROTO, None)),
        check_vma=False,
    )
```
